256 devices in a mesh: row: 8 (over z), col: 8 (over x_lo, y), layer: 4 (over x_hi, core).
Axes of the slice: x: 4 (x_hi: 2, x_lo: 2; x = x_hi * 2 + x_lo), y: 4, z: 8, core: 2. Of those that a mesh axis runs over, the one named last changes fastest.
Arguments:
- tokens: bfloat16 [5120, 6144], P('row', 'layer'), may hold values from -6 to 6
- expert_ids: int32 [5120, 2], replicated, may hold values from 0 to 7, all different within a row; in each aligned block of 5120 rows (0 to 5119, 5120 to 10239, ...) at most 2560 rows name the same one
- w_gate: bfloat16 [2, 6144, 8192], P(None, 'layer', ('row', 'col')), may hold values from -0.078125 to 0.078125
- w_up: bfloat16 [2, 6144, 8192], P(None, 'layer', ('row', 'col')), may hold values from -0.078125 to 0.078125
Outputs:
- hidden: bfloat16 [2, 2560, 8192], P(None, ('col', 'layer'), 'row')
The draws below stay inside these ranges and needn't reach their ends.
Inputs may be any that keep to these rules, and one draw needn't show every extreme that they name: `expert_ids`: each token names 2 different experts. No expert is named by more than 2560 tokens, a bound that some block reaches.
All inputs are finite; a program needn't handle non-finite values.
Results may differ from the reference program's by a relative error of at most 0.0012.
Values may be sent and summed in bfloat16 or wider, within the bound.
A program may use at most 128 MiB of HBM per device.

```python
import math
import jax
import jax.numpy as jnp
import numpy as np

D = 6144
EXPERTS = 8
TOP = 2
FF = 8192
EXP_FLIGHT = 2
SLOTS_DEV = 80
CAP = 2560
TOKENS = 5120
N_COL = 8
N_LAYER = 4


def block_scale(stream_key, extent, shards, low, top_value):
    def one(axis_at, shards_of):
        heights = jax.random.uniform(jax.random.fold_in(jax.random.fold_in(stream_key, 6), axis_at), (shards_of,), jnp.float32, low / len(shards), top_value / len(shards))
        return jnp.repeat(jnp.exp(heights), extent[axis_at] // shards_of).reshape((-1,) + (1,) * (len(extent) - axis_at - 1))

    factor_of = one(*shards[0])
    for cut in shards[1:]:
        factor_of = factor_of * one(*cut)
    return factor_of


def deal_out(rng, own, number, rows, number_of, top, most, slope):
    order = jax.random.permutation(rng, number_of)
    heavy_load, ordinary = load_shares(number_of, rows * top, most, slope, True), load_shares(number_of, rows * top, most, slope, False)
    places = jnp.arange(number_of)

    def named(lengths, offset_by):
        used = int((lengths > 0).sum())
        fixed = max(1, used // 4)
        passed = fixed + (places - fixed + offset_by * (used - fixed)) % max(1, number_of - fixed)
        return jnp.zeros((number_of,), jnp.int32).at[order[jnp.where(places < fixed, places, passed)]].set(jnp.asarray(lengths, jnp.int32))

    lengths = jnp.where(number % 4 == 0, named(heavy_load, number // 4), named(ordinary, number - number // 4 - 1))
    mixed = jax.random.permutation(jax.random.fold_in(own, 3), number_of)
    giver, receiver = mixed[0:number_of // 2 * 2:2], mixed[1:number_of // 2 * 2:2]
    room = jnp.minimum(lengths[giver] - 1, most - lengths[receiver]) // 2
    room = jnp.where((giver == order[0]) | (receiver == order[0]) | (lengths[receiver] == 0), 0, jnp.maximum(room, 0))
    passed = jax.random.randint(jax.random.fold_in(own, 4), (number_of // 2,), 0, 1 << 20) % (room + 1)
    lengths = lengths.at[giver].add(-passed).at[receiver].add(passed)
    members = jnp.searchsorted(jnp.cumsum(lengths), jnp.arange(rows * top), side="right").astype(jnp.int32)
    listing = members.reshape(top, rows).T
    listing = listing[jax.random.permutation(jax.random.fold_in(own, 1), rows)]
    offset_by = jax.random.randint(jax.random.fold_in(own, 2), (rows, 1), 0, top)
    return jnp.take_along_axis(listing, (jnp.arange(top)[None, :] + offset_by) % top, axis=1)


def load_shares(number_of, total, reach, slope, full):
    weights = [(1 << 20) // math.isqrt(standing ** slope) + 1 for standing in range(1, number_of + 1)]
    largest = reach if full else min(reach, max(-(-total // number_of), total * weights[0] // sum(weights)))
    least = 1 if total - largest >= number_of - 1 else 0
    given, surplus = [largest] + [least] * (number_of - 1), total - largest - least * (number_of - 1)
    while surplus > 0:
        candidates = [i for i in range(1, number_of) if given[i] < largest] or [i for i in range(1, number_of) if given[i] < reach]
        whole, remaining = sum([weights[i] for i in candidates]), surplus
        for i in candidates:
            addition = min(reach - given[i], max(1, remaining * weights[i] // whole), surplus)
            given[i] = given[i] + addition
            surplus = surplus - addition
    return np.array(given)


def centred(key, dims, scale, limit, shards=(), kind=jnp.bfloat16):
    loudness = block_scale(key, dims, shards, -0.22, 0.18) if shards else 1.0
    entries = jax.random.normal(key, dims, jnp.float32) * scale * loudness
    return jnp.minimum(jnp.maximum(entries, -limit), limit).astype(kind)


def setup_inputs(seed: int = 0) -> dict:
    streams_of = jax.random.split(jax.random.key(seed), 5)
    tokens = centred(streams_of[0], (TOKENS, D), 1.0, 6.0, ((0, 8), (1, 4)))
    expert_ids_keys = jax.random.split(jax.random.fold_in(streams_of[1], 1), TOKENS // TOKENS)
    expert_ids_turns = jax.random.permutation(jax.random.fold_in(streams_of[1], 3), TOKENS // TOKENS)
    expert_ids = jax.vmap(lambda own, number: deal_out(jax.random.fold_in(streams_of[1], 2), own, number, TOKENS, EXPERTS, TOP, CAP, 2))(expert_ids_keys, expert_ids_turns).reshape((TOKENS, TOP))
    w_gate = centred(streams_of[2], (EXP_FLIGHT, D, FF), D ** -0.5, 0.078125, ((1, 4), (2, 64)))
    w_up = centred(streams_of[3], (EXP_FLIGHT, D, FF), D ** -0.5, 0.078125, ((1, 4), (2, 64)))
    return {"tokens": tokens, "expert_ids": expert_ids, "w_gate": w_gate, "w_up": w_up}


def reference(tokens, expert_ids, w_gate, w_up):
    tok_count = tokens.shape[0]
    capacity = SLOTS_DEV * N_COL * N_LAYER
    expert_range = jnp.arange(EXP_FLIGHT, dtype=jnp.int32)
    member = jnp.any(expert_ids[:, :, None] == expert_range[None, None, :], axis=1).astype(jnp.int32)
    slot_rank = (jnp.cumsum(member, axis=0) - member).astype(jnp.int32)
    target = jnp.where(member > 0, slot_rank, capacity).astype(jnp.int32)
    token_range = jnp.broadcast_to(jnp.arange(tok_count, dtype=jnp.int32)[:, None], target.shape)
    slot_table = jnp.zeros((EXP_FLIGHT, capacity + 1), jnp.int32).at[expert_range[None, :], target].set(token_range)
    counts = jnp.sum(member, axis=0).astype(jnp.int32)
    live_mask = jnp.arange(capacity, dtype=jnp.int32)[None, :] < counts[:, None]
    results = []
    for expert in range(EXP_FLIGHT):
        slot_rows = jnp.where(live_mask[expert][:, None], tokens[slot_table[expert, :capacity]], jnp.zeros((), tokens.dtype))
        gate = jnp.dot(slot_rows, w_gate[expert], preferred_element_type=jnp.float32)
        up_part = jnp.dot(slot_rows, w_up[expert], preferred_element_type=jnp.float32)
        results.append((jax.nn.silu(gate) * up_part).astype(jnp.bfloat16))
    return jnp.stack(results)
```

```python
import functools

import jax
import jax.numpy as jnp
from jax import lax
from jax.experimental import pallas as pl
from jax.experimental.pallas import tpu as pltpu
from jax.sharding import PartitionSpec as P

MESH = pl.DeviceIdType.MESH
ROWS = 8
BLOCK = 80
HALF = 768
LANES = 128
EXPERTS = 2


def ring_steps(first):
    return (4, 3) if first else (3, 4)


def kernel(
    rank_ref, tok_ref, wg_ref, wu_ref, out_ref,
    wbuf, placed, sums, slots, part, from_core, from_hi, sent, back,
    w_s, w_r, rs_s, rs_r, x_s, x_r, ag_s, ag_r, c_s, c_r, h_s, h_r, o_s, o_r,
):
    z = lax.axis_index("row")
    col = lax.axis_index("col")
    layer = lax.axis_index("layer")
    xl, y = col // 4, col % 4
    xh, core = layer // 2, layer % 2

    def at_row(step):
        return (lax.rem(z + step + ROWS, ROWS), col, layer)

    def at_y(step):
        return (z, xl * 4 + lax.rem(y + step, 4), layer)

    pair = (z, (1 - xl) * 4 + y, layer)
    other_core = (z, col, xh * 2 + (1 - core))
    other_hi = (z, col, (1 - xh) * 2 + core)
    y_steps = (1, 3, 2)

    barrier = pltpu.get_barrier_semaphore()
    partners = [at_row(1), at_row(-1), at_y(1), at_y(2), at_y(3), pair, other_core, other_hi]
    for partner in partners:
        pl.semaphore_signal(barrier, inc=1, device_id=partner, device_id_type=MESH)
    pl.semaphore_wait(barrier, len(partners))

    pending = []

    def send(src, dst, send_sem, recv_sem, device):
        copy = pltpu.make_async_remote_copy(
            src_ref=src, dst_ref=dst, send_sem=send_sem, recv_sem=recv_sem,
            device_id=device, device_id_type=MESH,
        )
        copy.start()
        pending.append(copy)
        return copy

    w_copies = {}

    def send_weights(e):
        for d, step in enumerate(y_steps):
            for g, ref in enumerate((wg_ref, wu_ref)):
                w_copies[e, d, g] = send(
                    ref.at[e], wbuf.at[y, e, :, pl.ds(g * LANES, LANES)],
                    w_s.at[e, d, g], w_r.at[e, d, g], at_y(step),
                )

    send_weights(0)

    rs_copies = {}

    def owner_rows(ref, e, k):
        start = pl.multiple_of((k // 2) * BLOCK, 16)
        return ref.at[e, k % 2, pl.ds(start, BLOCK), :]

    def reduce_step(e, s):
        for d, sign in enumerate((1, -1)):
            steps = ring_steps(e == 0)[d]
            if s > steps:
                continue
            k = lax.rem(z + sign * (steps - s + 1) + ROWS, ROWS)
            if s == 1:
                src = owner_rows(placed, e, k)
            else:
                rs_copies[e, d, s - 1].wait_recv()
                src = sums.at[e, d, s - 2]
                src[...] = src[...] + owner_rows(placed, e, k)[...]
            rs_copies[e, d, s] = send(
                src, sums.at[e, d, s - 1], rs_s.at[e, d, s - 1], rs_r.at[e, d, s - 1], at_row(sign)
            )

    for e in range(EXPERTS):
        base = col * (4 * BLOCK)
        place = lax.broadcasted_iota(jnp.int32, (4 * BLOCK, tok_ref.shape[0]), 0) + base
        pick = (place == rank_ref[pl.ds(e, 1), :]).astype(jnp.float32).astype(jnp.bfloat16)
        for f in range(2):
            placed[e, f] = jnp.dot(
                pick, tok_ref[:, f * HALF : (f + 1) * HALF], preferred_element_type=jnp.float32
            ).astype(jnp.bfloat16)
        reduce_step(e, 1)

    for e in range(EXPERTS):
        wbuf[y, e, :, 0:LANES] = wg_ref[e]
        wbuf[y, e, :, LANES : 2 * LANES] = wu_ref[e]

    for s in range(2, 5):
        for e in range(EXPERTS):
            reduce_step(e, s)

    def slot_rows(e, k, half):
        start = pl.multiple_of((k // 2) * (2 * BLOCK) + half * BLOCK, 16)
        return slots.at[e, k % 2, pl.ds(start, BLOCK), :]

    x_copies = {}

    def finish_reduce(e):
        up, down = ring_steps(e == 0)
        rs_copies[e, 0, up].wait_recv()
        rs_copies[e, 1, down].wait_recv()
        total = sums[e, 0, up - 1] + sums[e, 1, down - 1] + owner_rows(placed, e, z)[...]
        mine = slot_rows(e, z, xl)
        mine[...] = total
        x_copies[e] = send(mine, mine, x_s.at[e], x_r.at[e], pair)

    ag_copies = {}

    def gather_step(e, h, s):
        half = xl if h == 0 else 1 - xl
        for d, sign in enumerate((1, -1)):
            if s > ring_steps(h == 0)[d]:
                continue
            k = lax.rem(z - sign * (s - 1) + ROWS, ROWS)
            if s > 1:
                ag_copies[e, h, d, s - 1].wait_recv()
            rows = slot_rows(e, k, half)
            ag_copies[e, h, d, s] = send(
                rows, rows, ag_s.at[e, h, d, s - 1], ag_r.at[e, h, d, s - 1], at_row(sign)
            )

    def gather_done(e):
        for h in range(2):
            for d in range(2):
                ag_copies[e, h, d, ring_steps(h == 0)[d]].wait_recv()

    def project(e):
        @pl.loop(0, 4)
        def _(b):
            total = jnp.dot(
                slots[e, 0], wbuf[b, e, 0:HALF, :], preferred_element_type=jnp.float32
            ) + jnp.dot(
                slots[e, 1], wbuf[b, e, HALF : 2 * HALF, :], preferred_element_type=jnp.float32
            )
            for a in range(4):
                for side in range(2):
                    start = (a * 2 + side) * BLOCK
                    part[e, a % 2, a // 2, side, b] = total[start : start + BLOCK]

    c_copies, h_copies, o_copies = {}, {}, {}

    def to_core(e):
        for i, hi in enumerate((1 - xh, xh)):
            c_copies[e, i] = send(
                part.at[e, 1 - core, hi], from_core.at[e, hi], c_s.at[e, i], c_r.at[e, i], other_core
            )

    def to_hi(e):
        c_copies[e, 0].wait_recv()
        src = part.at[e, core, 1 - xh]
        for side in range(2):
            for b in range(4):
                src[side, b] = src[side, b] + from_core[e, 1 - xh, side, b]
        h_copies[e] = send(src, from_hi.at[e], h_s.at[e], h_r.at[e], other_hi)

    def finish(e):
        c_copies[e, 1].wait_recv()
        h_copies[e].wait_recv()

        def hidden(side, b):
            total = part[e, core, xh, side, b] + from_core[e, xh, side, b] + from_hi[e, side, b]
            gate, up = total[:, :LANES], total[:, LANES:]
            return (gate / (1.0 + jnp.exp(-gate)) * up).astype(jnp.bfloat16)

        for b in range(4):
            sent[e, :, b * LANES : (b + 1) * LANES] = hidden(1 - xl, b)
        o_copies[e] = send(sent.at[e], back.at[e], o_s.at[e], o_r.at[e], pair)
        for b in range(4):
            start = pl.multiple_of((xl * 4 + b) * LANES, LANES)
            out_ref[e, :, pl.ds(start, LANES)] = hidden(xl, b)

    def weights_done(e):
        for d in range(3):
            for g in range(2):
                w_copies[e, d, g].wait_recv()

    finish_reduce(0)
    gather_step(0, 0, 1)
    send_weights(1)
    finish_reduce(1)
    x_copies[0].wait_recv()
    gather_step(0, 1, 1)
    for s in (2, 3):
        gather_step(0, 0, s)
        gather_step(0, 1, s)
    gather_step(1, 0, 1)
    x_copies[1].wait_recv()
    gather_step(1, 1, 1)
    gather_step(0, 0, 4)
    gather_step(0, 1, 4)
    gather_step(1, 0, 2)
    gather_step(1, 1, 2)
    gather_done(0)
    weights_done(0)
    project(0)
    to_core(0)
    gather_step(1, 0, 3)
    gather_step(1, 1, 3)
    to_hi(0)
    gather_step(1, 0, 4)
    gather_step(1, 1, 4)
    gather_done(1)
    weights_done(1)
    project(1)
    to_core(1)
    to_hi(1)
    finish(0)
    finish(1)
    for e in range(EXPERTS):
        o_copies[e].wait_recv()
        start = pl.multiple_of((1 - xl) * 4 * LANES, LANES)
        out_ref[e, :, pl.ds(start, 4 * LANES)] = back[e]
    for copy in pending:
        copy.wait_send()


def ranks(expert_ids, rows):
    tokens = expert_ids.shape[0]
    ids = expert_ids.T.reshape(2, tokens // LANES, LANES)
    experts = jnp.arange(EXPERTS, dtype=jnp.int32)[:, None, None]
    member = (ids[0][None] == experts) | (ids[1][None] == experts)
    ones = member.astype(jnp.bfloat16)
    lane = jnp.arange(LANES)
    before = (lane[:, None] < lane[None, :]).astype(jnp.bfloat16)
    within = jnp.einsum("erk,kl->erl", ones, before, preferred_element_type=jnp.float32)
    counts = jnp.sum(member.astype(jnp.float32), axis=2)
    line = jnp.arange(tokens // LANES)
    ahead = jnp.sum(jnp.where(line[None, :, None] > line[None, None, :], counts[:, None, :], 0.0), axis=2)
    rank = jnp.where(member, (within + ahead[:, :, None]).astype(jnp.int32), -1)
    start = lax.axis_index("row") * (rows // LANES)
    return lax.dynamic_slice_in_dim(rank, start, rows // LANES, 1).reshape(EXPERTS, rows)


def shards(tokens, expert_ids, w_gate, w_up):
    rank = ranks(expert_ids, tokens.shape[0])
    bf16, f32 = jnp.bfloat16, jnp.float32
    vmem, dma = pltpu.VMEM, pltpu.SemaphoreType.DMA
    return pl.pallas_call(
        kernel,
        name="experts",
        out_shape=jax.ShapeDtypeStruct((EXPERTS, BLOCK, 1024), bf16),
        in_specs=[pl.BlockSpec(memory_space=pltpu.VMEM)] * 4,
        out_specs=pl.BlockSpec(memory_space=pltpu.VMEM),
        scratch_shapes=[
            vmem((4, EXPERTS, 2 * HALF, 2 * LANES), bf16),
            vmem((EXPERTS, 2, 4 * BLOCK, HALF), bf16),
            vmem((EXPERTS, 2, 4, BLOCK, HALF), bf16),
            vmem((EXPERTS, 2, 8 * BLOCK, HALF), bf16),
            vmem((EXPERTS, 2, 2, 2, 4, BLOCK, 2 * LANES), f32),
            vmem((EXPERTS, 2, 2, 4, BLOCK, 2 * LANES), f32),
            vmem((EXPERTS, 2, 4, BLOCK, 2 * LANES), f32),
            vmem((EXPERTS, BLOCK, 4 * LANES), bf16),
            vmem((EXPERTS, BLOCK, 4 * LANES), bf16),
            dma((EXPERTS, 3, 2)), dma((EXPERTS, 3, 2)),
            dma((EXPERTS, 2, 4)), dma((EXPERTS, 2, 4)),
            dma((EXPERTS,)), dma((EXPERTS,)),
            dma((EXPERTS, 2, 2, 4)), dma((EXPERTS, 2, 2, 4)),
            dma((EXPERTS, 2)), dma((EXPERTS, 2)),
            dma((EXPERTS,)), dma((EXPERTS,)),
            dma((EXPERTS,)), dma((EXPERTS,)),
        ],
        compiler_params=pltpu.CompilerParams(
            collective_id=0, has_side_effects=True, vmem_limit_bytes=60 * 1024 * 1024
        ),
    )(rank, tokens, w_gate, w_up)


def solution(mesh):
    in_specs = (
        P("row", "layer"),
        P(),
        P(None, "layer", ("row", "col")),
        P(None, "layer", ("row", "col")),
    )
    out_specs = P(None, ("col", "layer"), "row")
    return jax.shard_map(shards, mesh=mesh, in_specs=in_specs, out_specs=out_specs, check_vma=False)
```

```python
import jax
import jax.numpy as jnp
from jax import lax
from jax.experimental import pallas as pl
from jax.experimental.pallas import tpu as pltpu
from jax.sharding import PartitionSpec as P

MESH = pl.DeviceIdType.MESH
ROWS = 8
BLOCK = 80
DEPTH = 1536
QUARTER = DEPTH // 4
HALF = DEPTH // 2
LANES = 128
EXPERTS = 2
CHUNKS = ((0, 0), (1, 0), (0, 1), (1, 1))
SIDEWAYS = (0,)
Y_STEP = (0, 1, 3, 2)
PIECES = ((0, 3), (3, 1))


def ring_steps(odd):
    return (3, 4) if odd else (4, 3)


class Copy:
    def __init__(self, src, dst, send_sem, recv_sem, device):
        self.copy = pltpu.make_async_remote_copy(
            src_ref=src, dst_ref=dst, send_sem=send_sem, recv_sem=recv_sem,
            device_id=device, device_id_type=MESH,
        )
        self.copy.start()
        self.arrived = False

    def wait(self):
        if not self.arrived:
            self.copy.wait_recv()
        self.arrived = True


def kernel(
    ids_ref, tok_ref, wg_ref, wu_ref, out_ref,
    wbuf, placed, sums, slots, part, from_core, from_hi, sent, back,
    w_s, w_r, wf_s, wf_r, rs_s, rs_r, x_s, x_r, ag_s, ag_r, c_s, c_r, h_s, h_r, o_s, o_r,
):
    z = lax.axis_index("row")
    col = lax.axis_index("col")
    layer = lax.axis_index("layer")
    xl, y = col // 4, col % 4
    xh, core = layer // 2, layer % 2

    def at_row(step):
        return (lax.rem(z + step + ROWS, ROWS), col, layer)

    def at_y(step):
        return (z, xl * 4 + lax.rem(y + step, 4), layer)

    pair = (z, (1 - xl) * 4 + y, layer)
    other_core = (z, col, xh * 2 + (1 - core))
    other_hi = (z, col, (1 - xh) * 2 + core)

    barrier = pltpu.get_barrier_semaphore()
    partners = [at_row(1), at_row(-1), at_y(1), at_y(3), pair, other_core, other_hi]
    for partner in partners:
        pl.semaphore_signal(barrier, inc=1, device_id=partner, device_id_type=MESH)
    pl.semaphore_wait(barrier, len(partners))

    copies = {}

    def send(key, src, dst, send_sem, recv_sem, device):
        copies[key] = Copy(src, dst, send_sem, recv_sem, device)

    def send_weights(e):
        for i in range(2):
            for d in range(2):
                half = i if d == 0 else 1 - i
                rows = pl.ds(half * HALF, HALF)
                for g, ref in enumerate((wg_ref, wu_ref)):
                    send(
                        ("w", e, d, half, g), ref.at[e, rows, :],
                        wbuf.at[2 - d, e, rows, pl.ds(g * LANES, LANES)],
                        w_s.at[e, d, half, g], w_r.at[e, d, half, g], at_y(1 if d == 0 else 3),
                    )

    def pass_weights(e):
        for d in range(2):
            for g in range(2):
                copies["w", e, d, d, g].wait()
            rows = pl.ds(d * HALF, HALF)
            send(
                ("f", e, d), wbuf.at[2 - d, e, rows, :], wbuf.at[3, e, rows, :],
                wf_s.at[e, d], wf_r.at[e, d], at_y(1 if d == 0 else 3),
            )

    def own_weights(e):
        wbuf[0, e, :, 0:LANES] = wg_ref[e]
        wbuf[0, e, :, LANES : 2 * LANES] = wu_ref[e]

    def weights_done(e, piece):
        if piece == 0:
            for d in range(2):
                for half in range(2):
                    for g in range(2):
                        copies["w", e, d, half, g].wait()
        else:
            for d in range(2):
                copies["f", e, d].wait()

    count = tok_ref.shape[0]
    start = pl.multiple_of(z * count, LANES)
    rank = []

    def find_ranks():
        above = lax.broadcasted_iota(jnp.int32, (count, count), 0)
        right = lax.broadcasted_iota(jnp.int32, (count, count), 1)
        before = (above < right).astype(jnp.float32).astype(jnp.bfloat16)
        token = lax.broadcasted_iota(jnp.int32, (1, ids_ref.shape[1]), 1)
        for e in range(EXPERTS):
            named = (ids_ref[0:1, :] == e) | (ids_ref[1:2, :] == e)
            ahead = jnp.sum((named & (token < start)).astype(jnp.float32), axis=1, keepdims=True)
            here = pl.ds(start, count)
            own = (ids_ref[0:1, here] == e) | (ids_ref[1:2, here] == e)
            ones = jnp.broadcast_to(own.astype(jnp.float32), (16, count)).astype(jnp.bfloat16)
            within = jnp.dot(ones, before, preferred_element_type=jnp.float32)[0:1]
            rank.append(jnp.where(own, (within + ahead).astype(jnp.int32), -1))

    def slot_start(c, r):
        to_hi = xh if CHUNKS[c][1] else 1 - xh
        to_core = core if r else 1 - core
        return (col * 4 + to_hi * 2 + to_core) * BLOCK

    def place_rows(c):
        index = lax.broadcasted_iota(jnp.int32, (BLOCK, count), 0)
        slot = jnp.concatenate([index + slot_start(c, 0), index + slot_start(c, 1)], axis=0)
        pick = (slot == rank[CHUNKS[c][0]]).astype(jnp.float32).astype(jnp.bfloat16)
        for f in range(2):
            placed[c, :, f * HALF : (f + 1) * HALF] = jnp.dot(
                pick, tok_ref[:, f * HALF : (f + 1) * HALF], preferred_element_type=jnp.float32
            ).astype(jnp.bfloat16)

    def owner_lanes(k):
        return pl.ds(pl.multiple_of((k % 4) * QUARTER, LANES), QUARTER)

    def owner_rows(c, k):
        return placed.at[c, pl.ds(pl.multiple_of((k // 4) * BLOCK, 16), BLOCK), owner_lanes(k)]

    def reduce_step(c, s):
        for d, sign in enumerate((1, -1)):
            steps = ring_steps(c % 2)[d]
            if s > steps:
                continue
            k = lax.rem(z + sign * (steps - s + 1) + ROWS, ROWS)
            if s == 1:
                src = owner_rows(c, k)
            else:
                copies["r", c, d, s - 1].wait()
                src = sums.at[c, d, s - 2]
                src[...] = src[...] + owner_rows(c, k)[...]
            send(
                ("r", c, d, s), src, sums.at[c, d, s - 1],
                rs_s.at[c, d, s - 1], rs_r.at[c, d, s - 1], at_row(sign),
            )

    def slot_rows(c, k, side):
        first = pl.multiple_of((k // 4) * (2 * BLOCK) + side * BLOCK, 16)
        return slots.at[c, pl.ds(first, BLOCK), owner_lanes(k)]

    def both_sides(c, k):
        first = pl.multiple_of((k // 4) * (2 * BLOCK), 16)
        return slots.at[c, pl.ds(first, 2 * BLOCK), owner_lanes(k)]

    def to_pair(c, i, k):
        rows = slot_rows(c, k, xl)
        send(("x", c, i), rows, rows, x_s.at[c, i], x_r.at[c, i], pair)

    def finish_reduce(c):
        up, down = ring_steps(c % 2)
        copies["r", c, 0, up].wait()
        copies["r", c, 1, down].wait()
        mine = slot_rows(c, z, xl)
        mine[...] = sums[c, 0, up - 1] + sums[c, 1, down - 1] + owner_rows(c, z)[...]
        if c in SIDEWAYS:
            gather_step(c, 1)
        else:
            to_pair(c, 0, z)

    def gather_step(c, s):
        if s == 1:
            if c in SIDEWAYS:
                to_pair(c, 0, z)
            else:
                copies["x", c, 0].wait()
        for d, sign in enumerate((1, -1)):
            steps = ring_steps(1 - c % 2)[d]
            if s - 1 > steps:
                continue
            k = lax.rem(z - sign * (s - 1) + ROWS, ROWS)
            if s > 1:
                copies["a", c, d, s - 1].wait()
            if s <= steps:
                rows = slot_rows(c, k, xl) if c in SIDEWAYS else both_sides(c, k)
                send(
                    ("a", c, d, s), rows, rows,
                    ag_s.at[c, d, s - 1], ag_r.at[c, d, s - 1], at_row(sign),
                )
            if s > 1 and c in SIDEWAYS:
                to_pair(c, 1 + d * ring_steps(1 - c % 2)[0] + s - 2, k)

    def slots_done(c):
        gather_step(c, 5)
        if c in SIDEWAYS:
            for i in range(8):
                copies["x", c, i].wait()

    def project(c, piece, r=None):
        e = CHUNKS[c][0]
        first, number = PIECES[piece]
        rows = range(2) if r is None else (r,)
        top = rows[0] * 2 * BLOCK
        span = len(rows) * 2 * BLOCK

        @pl.loop(first, first + number)
        def _(b):
            total = jnp.dot(
                slots[c, top : top + span, :], wbuf[b, e], preferred_element_type=jnp.float32
            )
            for i, row in enumerate(rows):
                for side in range(2):
                    at = (i * 2 + side) * BLOCK
                    part[c, row, b, side] = total[at : at + BLOCK]

    def to_core(c, piece):
        here = pl.ds(*PIECES[piece])
        send(
            ("c", c, piece), part.at[c, 0, here], from_core.at[c, here],
            c_s.at[c, piece], c_r.at[c, piece], other_core,
        )

    def to_hi(c, piece):
        e = CHUNKS[c][0]
        first, number = PIECES[piece]
        copies["c", c, piece].wait()

        @pl.loop(first, first + number)
        def _(b):
            for side in range(2):
                part[c, 1, b, side] = part[c, 1, b, side] + from_core[c, b, side]

        here = pl.ds(first, number)
        send(
            ("h", e, piece), part.at[c, 1, here], from_hi.at[e, here],
            h_s.at[e, piece], h_r.at[e, piece], other_hi,
        )

    def finish(e):
        c = CHUNKS.index((e, 1))
        for piece in range(2):
            copies["h", e, piece].wait()
        for piece in range(2):
            copies["c", c, piece].wait()

        def hidden(side, b):
            total = part[c, 1, b, side] + from_core[c, b, side] + from_hi[e, b, side]
            gate, up = total[:, :LANES], total[:, LANES:]
            return (gate / (1.0 + jnp.exp(-gate)) * up).astype(jnp.bfloat16)

        for b in range(4):
            sent[e, :, b * LANES : (b + 1) * LANES] = hidden(1 - xl, b)
        send(("o", e), sent.at[e], back.at[e], o_s.at[e], o_r.at[e], pair)
        for b in range(4):
            out_ref[e, :, out_lanes(xl, b)] = hidden(xl, b)

    def out_lanes(side, b):
        return pl.ds(pl.multiple_of((side * 4 + lax.rem(y + Y_STEP[b], 4)) * LANES, LANES), LANES)

    def take_back(e):
        copies["o", e].wait()
        for b in range(4):
            out_ref[e, :, out_lanes(1 - xl, b)] = back[e, :, b * LANES : (b + 1) * LANES]

    def project_all(c):
        for piece in range(2):
            weights_done(CHUNKS[c][0], piece)
            project(c, piece)
            to_core(c, piece)

    def project_rows(c):
        for piece in range(2):
            weights_done(CHUNKS[c][0], piece)
        for r in range(2):
            for piece in range(2):
                project(c, piece, r)
                if r == 0:
                    to_core(c, piece)

    plan = [
        (0.0, send_weights, 0),
        (0.1, find_ranks),
        (2.2, own_weights, 0),
        (4.4, own_weights, 1),
        (10.5, pass_weights, 0),
        (13.0, send_weights, 1),
        (37.0, pass_weights, 1),
    ]
    first_reduce = (1.0, 1.5, 9.0, 15.0)
    reduce_gap = (3.2, 3.2, 3.2, 3.2)
    first_gather = (14.5, 18.0, 31.0, 40.0)
    gather_gap = (3.2, 4.4, 4.4, 4.4)
    for c in range(4):
        plan.append((first_reduce[c] - 0.1, place_rows, c))
        for s in range(1, 5):
            plan.append((first_reduce[c] + (s - 1) * reduce_gap[c], reduce_step, c, s))
        plan.append((first_reduce[c] + 4 * reduce_gap[c], finish_reduce, c))
        for s in range(1 + (c in SIDEWAYS), 5):
            plan.append((first_gather[c] + (s - 1) * gather_gap[c], gather_step, c, s))
    plan += [
        (31.0, slots_done, 0), (31.1, project_all, 0), (34.0, to_hi, 0, 0), (34.5, to_hi, 0, 1),
        (38.0, slots_done, 1), (43.0, weights_done, 1, 0), (43.1, project, 1, 0), (43.2, to_core, 1, 0),
        (46.0, to_hi, 1, 0),
        (50.0, slots_done, 2), (50.1, project_all, 2),
        (51.0, weights_done, 1, 1), (51.1, project, 1, 1), (51.2, to_core, 1, 1), (52.5, to_hi, 1, 1),
        (55.0, finish, 0),
        (59.0, slots_done, 3), (59.1, project_rows, 3), (62.0, finish, 1),
        (64.0, take_back, 0), (65.0, take_back, 1),
    ]
    for _, act, *args in sorted(plan, key=lambda step: step[0]):
        act(*args)
    for copy in copies.values():
        copy.copy.wait_send()


def shards(tokens, expert_ids, w_gate, w_up):
    bf16, f32 = jnp.bfloat16, jnp.float32
    vmem, dma = pltpu.VMEM, pltpu.SemaphoreType.DMA
    chunks = len(CHUNKS)
    return pl.pallas_call(
        kernel,
        name="experts",
        out_shape=jax.ShapeDtypeStruct((EXPERTS, BLOCK, 1024), bf16),
        in_specs=[pl.BlockSpec(memory_space=pltpu.VMEM)] * 4,
        out_specs=pl.BlockSpec(memory_space=pltpu.VMEM),
        scratch_shapes=[
            vmem((4, EXPERTS, DEPTH, 2 * LANES), bf16),
            vmem((chunks, 2 * BLOCK, DEPTH), bf16),
            vmem((chunks, 2, 4, BLOCK, QUARTER), bf16),
            vmem((chunks, 4 * BLOCK, DEPTH), bf16),
            vmem((chunks, 2, 4, 2, BLOCK, 2 * LANES), f32),
            vmem((chunks, 4, 2, BLOCK, 2 * LANES), f32),
            vmem((EXPERTS, 4, 2, BLOCK, 2 * LANES), f32),
            vmem((EXPERTS, BLOCK, 4 * LANES), bf16),
            vmem((EXPERTS, BLOCK, 4 * LANES), bf16),
            dma((EXPERTS, 2, 2, 2)), dma((EXPERTS, 2, 2, 2)),
            dma((EXPERTS, 2)), dma((EXPERTS, 2)),
            dma((chunks, 2, 4)), dma((chunks, 2, 4)),
            dma((chunks, 8)), dma((chunks, 8)),
            dma((chunks, 2, 4)), dma((chunks, 2, 4)),
            dma((chunks, 2)), dma((chunks, 2)),
            dma((EXPERTS, 2)), dma((EXPERTS, 2)),
            dma((EXPERTS,)), dma((EXPERTS,)),
        ],
        compiler_params=pltpu.CompilerParams(
            collective_id=0, has_side_effects=True, vmem_limit_bytes=60 * 1024 * 1024
        ),
    )(expert_ids.T, tokens, w_gate, w_up)


def solution(mesh):
    in_specs = (
        P("row", "layer"),
        P(),
        P(None, "layer", ("row", "col")),
        P(None, "layer", ("row", "col")),
    )
    out_specs = P(None, ("col", "layer"), "row")
    return jax.shard_map(shards, mesh=mesh, in_specs=in_specs, out_specs=out_specs, check_vma=False)
```

```python
import jax
import jax.numpy as jnp
from jax import lax
from jax.experimental import pallas as pl
from jax.experimental.pallas import tpu as pltpu
from jax.sharding import PartitionSpec as P

MESH = pl.DeviceIdType.MESH
ROWS = 8
BLOCK = 80
DEPTH = 1536
QUARTER = DEPTH // 4
HALF = DEPTH // 2
LANES = 128
EXPERTS = 2
CHUNKS = ((0, 0), (1, 0), (0, 1), (1, 1))
SIDEWAYS = (0, 1)
Y_STEP = (0, 1, 3, 2)
PIECES = ((0, 1), (1, 2), (3, 1))

PLAN = (
    "w11", "r001", "r111", "w01", "w00", "r011", "r002", "r112", "r101", "r012", "r003", "r113",
    "r102", "r013", "r004", "r114", "r103", "t0", "r311", "r301", "t1", "w10", "a012", "a002",
    "r211", "r201", "r312", "r302", "a102", "a003", "a013", "a112", "r212", "r202", "r303", "r313",
    "a014", "a103", "f00", "f01", "a113", "a004", "r203", "r314", "a015", "a104", "r213", "r204",
    "a114", "t3", "p010", "a105", "p011", "f11", "f10", "t2", "h01", "p0001", "a301", "a311",
    "h00", "p1101", "a201", "a211", "h11", "a302", "a312", "p0201", "h02", "a202", "a212", "a303",
    "a313", "a203", "a213", "p1201", "h12", "a304", "p100", "a214", "p101", "h10", "p320", "p3101",
    "p321", "p3001", "p220", "p2101", "p2001", "p221", "o0", "m0", "o1", "m1", "b0", "b1",
)


def ring_steps(odd):
    return (3, 4) if odd else (4, 3)


class Copy:
    def __init__(self, src, dst, send_sem, recv_sem, device):
        self.copy = pltpu.make_async_remote_copy(
            src_ref=src, dst_ref=dst, send_sem=send_sem, recv_sem=recv_sem,
            device_id=device, device_id_type=MESH,
        )
        self.copy.start()
        self.arrived = False

    def wait(self):
        if not self.arrived:
            self.copy.wait_recv()
        self.arrived = True


def kernel(
    ids_hbm, tok_hbm, wg_hbm, wu_hbm, out_ref,
    ids_ref, tok_ref, wbuf, placed, sums, slots, part, from_core, from_hi, sent, back,
    in_s, w_s, w_r, wf_s, wf_r, rs_s, rs_r, x_s, x_r, ag_s, ag_r, c_s, c_r, h_s, h_r, o_s, o_r,
):
    z = lax.axis_index("row")
    col = lax.axis_index("col")
    layer = lax.axis_index("layer")
    xl, y = col // 4, col % 4
    xh, core = layer // 2, layer % 2

    def at_row(step):
        return (lax.rem(z + step + ROWS, ROWS), col, layer)

    def at_y(step):
        return (z, xl * 4 + lax.rem(y + step, 4), layer)

    pair = (z, (1 - xl) * 4 + y, layer)
    other_core = (z, col, xh * 2 + (1 - core))
    other_hi = (z, col, (1 - xh) * 2 + core)

    barrier = pltpu.get_barrier_semaphore()
    partners = [at_row(1), at_row(-1), at_y(1), at_y(3), pair, other_core, other_hi]
    for partner in partners:
        pl.semaphore_signal(barrier, inc=1, device_id=partner, device_id_type=MESH)

    ids_in = pltpu.make_async_copy(ids_hbm, ids_ref, in_s.at[0])
    tok_in = pltpu.make_async_copy(tok_hbm, tok_ref, in_s.at[1])
    w_in = [
        [
            pltpu.make_async_copy(
                ref.at[e], wbuf.at[0, e, :, pl.ds(g * LANES, LANES)], in_s.at[2 + 2 * e + g]
            )
            for g, ref in enumerate((wg_hbm, wu_hbm))
        ]
        for e in range(EXPERTS)
    ]
    for copy in (ids_in, tok_in, *w_in[0], *w_in[1]):
        copy.start()

    copies = {}

    def send(key, src, dst, send_sem, recv_sem, device):
        copies[key] = Copy(src, dst, send_sem, recv_sem, device)

    def send_weights(e, i):
        for d in range(2):
            half = i if d == 0 else 1 - i
            rows = pl.ds(half * HALF, HALF)
            send(
                ("w", e, d, half), wbuf.at[0, e, rows, :], wbuf.at[2 - d, e, rows, :],
                w_s.at[e, d, half], w_r.at[e, d, half], at_y(1 if d == 0 else 3),
            )

    def pass_weights(e, d):
        copies["w", e, d, d].wait()
        rows = pl.ds(d * HALF, HALF)
        send(
            ("f", e, d), wbuf.at[2 - d, e, rows, :], wbuf.at[3, e, rows, :],
            wf_s.at[e, d], wf_r.at[e, d], at_y(1 if d == 0 else 3),
        )

    def weights_done(e, piece):
        if piece == 1:
            for d in range(2):
                for half in range(2):
                    copies["w", e, d, half].wait()
        elif piece == 2:
            for d in range(2):
                copies["f", e, d].wait()

    count = tok_ref.shape[0]
    start = pl.multiple_of(z * count, LANES)
    rank = []

    def find_ranks():
        above = lax.broadcasted_iota(jnp.int32, (count, count), 0)
        right = lax.broadcasted_iota(jnp.int32, (count, count), 1)
        before = (above < right).astype(jnp.float32).astype(jnp.bfloat16)
        token = lax.broadcasted_iota(jnp.int32, (1, ids_ref.shape[1]), 1)
        for e in range(EXPERTS):
            named = (ids_ref[0:1, :] == e) | (ids_ref[1:2, :] == e)
            ahead = jnp.sum((named & (token < start)).astype(jnp.float32), axis=1, keepdims=True)
            here = pl.ds(start, count)
            own = (ids_ref[0:1, here] == e) | (ids_ref[1:2, here] == e)
            ones = jnp.broadcast_to(own.astype(jnp.float32), (16, count)).astype(jnp.bfloat16)
            within = jnp.dot(ones, before, preferred_element_type=jnp.float32)[0:1]
            rank.append(jnp.where(own, (within + ahead).astype(jnp.int32), -1))

    def slot_start(c, r):
        to_hi = xh if CHUNKS[c][1] else 1 - xh
        to_core = core if r else 1 - core
        return (col * 4 + to_hi * 2 + to_core) * BLOCK

    def place_rows(c):
        index = lax.broadcasted_iota(jnp.int32, (BLOCK, count), 0)
        slot = jnp.concatenate([index + slot_start(c, 0), index + slot_start(c, 1)], axis=0)
        pick = (slot == rank[CHUNKS[c][0]]).astype(jnp.float32).astype(jnp.bfloat16)
        for f in range(2):
            placed[c, :, f * HALF : (f + 1) * HALF] = jnp.dot(
                pick, tok_ref[:, f * HALF : (f + 1) * HALF], preferred_element_type=jnp.float32
            ).astype(jnp.bfloat16)

    def owner_lanes(k):
        return pl.ds(pl.multiple_of((k % 4) * QUARTER, LANES), QUARTER)

    def owner_rows(c, k):
        return placed.at[c, pl.ds(pl.multiple_of((k // 4) * BLOCK, 16), BLOCK), owner_lanes(k)]

    def reduce_step(c, d, s):
        sign, steps = 1 - 2 * d, ring_steps(c % 2)[d]
        k = lax.rem(z + sign * (steps - s + 1) + ROWS, ROWS)
        if s == 1:
            src = owner_rows(c, k)
        else:
            copies["r", c, d, s - 1].wait()
            src = sums.at[c, d, s - 2]
            src[...] = src[...] + owner_rows(c, k)[...]
        send(
            ("r", c, d, s), src, sums.at[c, d, s - 1],
            rs_s.at[c, d, s - 1], rs_r.at[c, d, s - 1], at_row(sign),
        )

    def slot_rows(c, k, side):
        first = pl.multiple_of((k // 4) * (2 * BLOCK) + side * BLOCK, 16)
        return slots.at[c, pl.ds(first, BLOCK), owner_lanes(k)]

    def both_sides(c, k):
        first = pl.multiple_of((k // 4) * (2 * BLOCK), 16)
        return slots.at[c, pl.ds(first, 2 * BLOCK), owner_lanes(k)]

    def to_pair(c, i, k):
        rows = slot_rows(c, k, xl)
        send(("x", c, i), rows, rows, x_s.at[c, i], x_r.at[c, i], pair)

    def finish_reduce(c):
        up, down = ring_steps(c % 2)
        copies["r", c, 0, up].wait()
        copies["r", c, 1, down].wait()
        mine = slot_rows(c, z, xl)
        mine[...] = sums[c, 0, up - 1] + sums[c, 1, down - 1] + owner_rows(c, z)[...]
        if c in SIDEWAYS:
            for d in range(2):
                gather_send(c, d, 1)
        to_pair(c, 0, z)

    def gather_send(c, d, s):
        sign = 1 - 2 * d
        k = lax.rem(z - sign * (s - 1) + ROWS, ROWS)
        rows = slot_rows(c, k, xl) if c in SIDEWAYS else both_sides(c, k)
        send(
            ("a", c, d, s), rows, rows, ag_s.at[c, d, s - 1], ag_r.at[c, d, s - 1], at_row(sign)
        )

    def gather_step(c, d, s):
        sign, steps = 1 - 2 * d, ring_steps(1 - c % 2)
        if s == 1:
            copies["x", c, 0].wait()
        else:
            copies["a", c, d, s - 1].wait()
        if s <= steps[d]:
            gather_send(c, d, s)
        if c in SIDEWAYS:
            to_pair(c, 1 + d * steps[0] + s - 2, lax.rem(z - sign * (s - 1) + ROWS, ROWS))

    def slots_done(c):
        for d in range(2):
            copies["a", c, d, ring_steps(1 - c % 2)[d]].wait()
        for i in range(8 if c in SIDEWAYS else 1):
            copies["x", c, i].wait()

    def project(c, piece, *rows):
        e = CHUNKS[c][0]
        first, number = PIECES[piece]
        slots_done(c)
        weights_done(e, piece)
        top, span = rows[0] * 2 * BLOCK, len(rows) * 2 * BLOCK
        for b in range(first, first + number):
            total = jnp.dot(
                slots[c, top : top + span, :], wbuf[b, e], preferred_element_type=jnp.float32
            )
            for i, row in enumerate(rows):
                for side in range(2):
                    at = (i * 2 + side) * BLOCK
                    part[c, row, b, side] = total[at : at + BLOCK]
        if 0 in rows:
            here = pl.ds(first, number)
            send(
                ("c", c, piece), part.at[c, 0, here], from_core.at[c, here],
                c_s.at[c, piece], c_r.at[c, piece], other_core,
            )

    def to_hi(c, piece):
        e = CHUNKS[c][0]
        first, number = PIECES[piece]
        copies["c", c, piece].wait()

        for b in range(first, first + number):
            for side in range(2):
                part[c, 1, b, side] = part[c, 1, b, side] + from_core[c, b, side]

        here = pl.ds(first, number)
        send(
            ("h", e, piece), part.at[c, 1, here], from_hi.at[e, here],
            h_s.at[e, piece], h_r.at[e, piece], other_hi,
        )

    def hidden(e, side, b):
        c = CHUNKS.index((e, 1))
        total = part[c, 1, b, side] + from_core[c, b, side] + from_hi[e, b, side]
        gate, up = total[:, :LANES], total[:, LANES:]
        return (gate / (1.0 + jnp.exp(-gate)) * up).astype(jnp.bfloat16)

    def finish_out(e):
        c = CHUNKS.index((e, 1))
        for piece in range(len(PIECES)):
            copies["h", e, piece].wait()
            copies["c", c, piece].wait()
        for b in range(4):
            sent[e, :, b * LANES : (b + 1) * LANES] = hidden(e, 1 - xl, b)
        send(("o", e), sent.at[e], back.at[e], o_s.at[e], o_r.at[e], pair)

    def finish_own(e):
        for b in range(4):
            out_ref[e, :, out_lanes(xl, b)] = hidden(e, xl, b)

    def out_lanes(side, b):
        return pl.ds(pl.multiple_of((side * 4 + lax.rem(y + Y_STEP[b], 4)) * LANES, LANES), LANES)

    def take_back(e):
        copies["o", e].wait()
        for b in range(4):
            out_ref[e, :, out_lanes(1 - xl, b)] = back[e, :, b * LANES : (b + 1) * LANES]

    ids_in.wait()
    find_ranks()
    tok_in.wait()
    for c in range(len(CHUNKS)):
        place_rows(c)
    for e in range(EXPERTS):
        for copy in w_in[e]:
            copy.wait()
    pl.semaphore_wait(barrier, len(partners))
    acts = {
        "w": send_weights, "f": pass_weights, "r": reduce_step, "t": finish_reduce, "a": gather_step,
        "p": project, "h": to_hi, "o": finish_out, "m": finish_own, "b": take_back,
    }
    for step in PLAN:
        acts[step[0]](*map(int, step[1:]))
    for copy in copies.values():
        copy.copy.wait_send()


def shards(tokens, expert_ids, w_gate, w_up):
    bf16, f32 = jnp.bfloat16, jnp.float32
    vmem, dma = pltpu.VMEM, pltpu.SemaphoreType.DMA
    chunks = len(CHUNKS)
    return pl.pallas_call(
        kernel,
        name="experts",
        out_shape=jax.ShapeDtypeStruct((EXPERTS, BLOCK, 1024), bf16),
        in_specs=[pl.BlockSpec(memory_space=pl.ANY)] * 4,
        out_specs=pl.BlockSpec(memory_space=pltpu.VMEM),
        scratch_shapes=[
            vmem(expert_ids.shape[::-1], jnp.int32),
            vmem(tokens.shape, bf16),
            vmem((4, EXPERTS, DEPTH, 2 * LANES), bf16),
            vmem((chunks, 2 * BLOCK, DEPTH), bf16),
            vmem((chunks, 2, 4, BLOCK, QUARTER), bf16),
            vmem((chunks, 4 * BLOCK, DEPTH), bf16),
            vmem((chunks, 2, 4, 2, BLOCK, 2 * LANES), f32),
            vmem((chunks, 4, 2, BLOCK, 2 * LANES), f32),
            vmem((EXPERTS, 4, 2, BLOCK, 2 * LANES), f32),
            vmem((EXPERTS, BLOCK, 4 * LANES), bf16),
            vmem((EXPERTS, BLOCK, 4 * LANES), bf16),
            dma((6,)),
            dma((EXPERTS, 2, 2)), dma((EXPERTS, 2, 2)),
            dma((EXPERTS, 2)), dma((EXPERTS, 2)),
            dma((chunks, 2, 4)), dma((chunks, 2, 4)),
            dma((chunks, 8)), dma((chunks, 8)),
            dma((chunks, 2, 4)), dma((chunks, 2, 4)),
            dma((chunks, 3)), dma((chunks, 3)),
            dma((EXPERTS, 3)), dma((EXPERTS, 3)),
            dma((EXPERTS,)), dma((EXPERTS,)),
        ],
        compiler_params=pltpu.CompilerParams(
            collective_id=0, has_side_effects=True, vmem_limit_bytes=60 * 1024 * 1024
        ),
    )(expert_ids.T, tokens, w_gate, w_up)


def solution(mesh):
    in_specs = (
        P("row", "layer"),
        P(),
        P(None, "layer", ("row", "col")),
        P(None, "layer", ("row", "col")),
    )
    out_specs = P(None, ("col", "layer"), "row")
    return jax.shard_map(shards, mesh=mesh, in_specs=in_specs, out_specs=out_specs, check_vma=False)
```

```python
import jax
import jax.numpy as jnp
from jax import lax
from jax.experimental import pallas as pl
from jax.experimental.pallas import tpu as pltpu
from jax.sharding import PartitionSpec as P

MESH = pl.DeviceIdType.MESH
ROWS = 8
BLOCK = 80
DEPTH = 1536
QUARTER = DEPTH // 4
HALF = DEPTH // 2
LANES = 128
EXPERTS = 2
CHUNKS = ((0, 0), (1, 0), (0, 1), (1, 1))
TREES = (0,)
SPREADS = ()
SIDEWAYS = (0,)
Y_STEP = (0, 1, 3, 2)
PIECES = ((0, 1), (1, 2), (3, 1))

PLAN = (
    "r001", "r111", "r311", "r301", "w11", "w00", "w01", "r011", "r112", "r312", "r101", "r012",
    "r002", "r201", "r113", "r313", "r102", "r302", "t0", "r211", "r202", "r114", "r103", "r303",
    "a012", "a002", "r212", "f00", "f01", "r203", "t1", "a013", "r314", "r213", "a003", "a101",
    "r204", "a014", "t3", "a004", "a111", "a015", "w10", "a311", "a102", "a301", "t2", "p000",
    "a112", "p010", "p001", "p011", "h00", "a211", "a103", "a312", "h01", "p0201", "a302", "a113",
    "h02", "a104", "a212", "a201", "a303", "a313", "f11", "f10", "p1001", "p1101", "h10", "a202",
    "a213", "h11", "a304", "a203", "a214", "p120", "p300", "p3101", "p121", "h12", "p3201", "p301",
    "p2101", "p2001", "p2201", "o10", "m10", "o01", "m01", "o00", "o11", "o02", "m11", "m02",
    "m00", "b10", "o12", "m12", "b01", "b00", "b11", "b02", "b12",
)


def ring_steps(odd):
    return (3, 4) if odd else (4, 3)


class Copy:
    def __init__(self, src, dst, send_sem, recv_sem, device):
        self.copy = pltpu.make_async_remote_copy(
            src_ref=src, dst_ref=dst, send_sem=send_sem, recv_sem=recv_sem,
            device_id=device, device_id_type=MESH,
        )
        self.copy.start()
        self.arrived = False

    def wait(self):
        if not self.arrived:
            self.copy.wait_recv()
        self.arrived = True


def kernel(
    ids_hbm, tok_hbm, wg_hbm, wu_hbm, out_ref,
    ids_ref, tok_ref, wbuf, placed, sums, slots, part, from_core, from_hi, sent, back,
    in_s, w_s, w_r, wf_s, wf_r, rs_s, rs_r, x_s, x_r, ag_s, ag_r, c_s, c_r, h_s, h_r, o_s, o_r,
):
    z = lax.axis_index("row")
    col = lax.axis_index("col")
    layer = lax.axis_index("layer")
    xl, y = col // 4, col % 4
    xh, core = layer // 2, layer % 2

    def at_row(step):
        return (lax.rem(z + step + ROWS, ROWS), col, layer)

    def at_y(step):
        return (z, xl * 4 + lax.rem(y + step, 4), layer)

    pair = (z, (1 - xl) * 4 + y, layer)
    other_core = (z, col, xh * 2 + (1 - core))
    other_hi = (z, col, (1 - xh) * 2 + core)

    barrier = pltpu.get_barrier_semaphore()
    rows_met = (1, -1, 2, -2) if TREES or SPREADS else (1, -1)
    partners = [*map(at_row, rows_met), at_y(1), at_y(3), pair, other_core, other_hi]
    for partner in partners:
        pl.semaphore_signal(barrier, inc=1, device_id=partner, device_id_type=MESH)

    ids_in = pltpu.make_async_copy(ids_hbm, ids_ref, in_s.at[0])
    tok_in = pltpu.make_async_copy(tok_hbm, tok_ref, in_s.at[1])
    w_in = [
        [
            pltpu.make_async_copy(
                ref.at[e], wbuf.at[0, e, :, pl.ds(g * LANES, LANES)], in_s.at[2 + 2 * e + g]
            )
            for g, ref in enumerate((wg_hbm, wu_hbm))
        ]
        for e in range(EXPERTS)
    ]
    for copy in (ids_in, tok_in, *w_in[0], *w_in[1]):
        copy.start()

    copies = {}

    def send(key, src, dst, send_sem, recv_sem, device):
        copies[key] = Copy(src, dst, send_sem, recv_sem, device)

    def send_weights(e, i):
        for d in range(2):
            half = i if d == 0 else 1 - i
            rows = pl.ds(half * HALF, HALF)
            send(
                ("w", e, d, half), wbuf.at[0, e, rows, :], wbuf.at[2 - d, e, rows, :],
                w_s.at[e, d, half], w_r.at[e, d, half], at_y(1 if d == 0 else 3),
            )

    def pass_weights(e, d):
        copies["w", e, d, d].wait()
        rows = pl.ds(d * HALF, HALF)
        send(
            ("f", e, d), wbuf.at[2 - d, e, rows, :], wbuf.at[3, e, rows, :],
            wf_s.at[e, d], wf_r.at[e, d], at_y(1 if d == 0 else 3),
        )

    def weights_done(e, piece):
        if piece == 1:
            for d in range(2):
                for half in range(2):
                    copies["w", e, d, half].wait()
        elif piece == 2:
            for d in range(2):
                copies["f", e, d].wait()

    count = tok_ref.shape[0]
    start = pl.multiple_of(z * count, LANES)
    rank = []

    def find_ranks():
        above = lax.broadcasted_iota(jnp.int32, (count, count), 0)
        right = lax.broadcasted_iota(jnp.int32, (count, count), 1)
        before = (above < right).astype(jnp.float32).astype(jnp.bfloat16)
        token = lax.broadcasted_iota(jnp.int32, (1, ids_ref.shape[1]), 1)
        for e in range(EXPERTS):
            named = (ids_ref[0:1, :] == e) | (ids_ref[1:2, :] == e)
            ahead = jnp.sum((named & (token < start)).astype(jnp.float32), axis=1, keepdims=True)
            here = pl.ds(start, count)
            own = (ids_ref[0:1, here] == e) | (ids_ref[1:2, here] == e)
            ones = jnp.broadcast_to(own.astype(jnp.float32), (16, count)).astype(jnp.bfloat16)
            within = jnp.dot(ones, before, preferred_element_type=jnp.float32)[0:1]
            rank.append(jnp.where(own, (within + ahead).astype(jnp.int32), -1))

    def slot_start(c, r):
        to_hi = xh if CHUNKS[c][1] else 1 - xh
        to_core = core if r else 1 - core
        return (col * 4 + to_hi * 2 + to_core) * BLOCK

    def place_rows(c):
        index = lax.broadcasted_iota(jnp.int32, (BLOCK, count), 0)
        slot = jnp.concatenate([index + slot_start(c, 0), index + slot_start(c, 1)], axis=0)
        pick = (slot == rank[CHUNKS[c][0]]).astype(jnp.float32).astype(jnp.bfloat16)
        for f in range(2):
            placed[c, :, f * HALF : (f + 1) * HALF] = jnp.dot(
                pick, tok_ref[:, f * HALF : (f + 1) * HALF], preferred_element_type=jnp.float32
            ).astype(jnp.bfloat16)

    def owner_lanes(k):
        return pl.ds(pl.multiple_of((k % 4) * QUARTER, LANES), QUARTER)

    def owner_rows(c, k):
        return placed.at[c, pl.ds(pl.multiple_of((k // 4) * BLOCK, 16), BLOCK), owner_lanes(k)]

    def reduce_send(c, d, s, src, hops):
        send(
            ("r", c, d, s), src, sums.at[c, d, s - 1],
            rs_s.at[c, d, s - 1], rs_r.at[c, d, s - 1], at_row((1 - 2 * d) * hops),
        )

    def reduce_step(c, d, s):
        sign, steps = 1 - 2 * d, ring_steps(c % 2)[d]

        def rows_for(distance):
            return owner_rows(c, lax.rem(z + sign * distance + ROWS, ROWS))

        if c not in TREES:
            src = rows_for(steps - s + 1)
            if s > 1:
                copies["r", c, d, s - 1].wait()
                sums[c, d, s - 2] = sums[c, d, s - 2] + src[...]
                src = sums.at[c, d, s - 2]
            reduce_send(c, d, s, src, 1)
        elif s == 1:
            reduce_send(c, d, 1, rows_for(3), 1)
            if steps == 4:
                reduce_send(c, d, 2, rows_for(4), 2)
            reduce_send(c, d, 4, rows_for(1), 1)
        else:
            copies["r", c, d, 1].wait()
            total = sums[c, d, 0] + rows_for(2)[...]
            if steps == 4:
                copies["r", c, d, 2].wait()
                total = total + sums[c, d, 1]
            sums[c, d, 0] = total
            reduce_send(c, d, 3, sums.at[c, d, 0], 2)

    def slot_rows(c, k, side):
        first = pl.multiple_of((k // 4) * (2 * BLOCK) + side * BLOCK, 16)
        return slots.at[c, pl.ds(first, BLOCK), owner_lanes(k)]

    def both_sides(c, k):
        first = pl.multiple_of((k // 4) * (2 * BLOCK), 16)
        return slots.at[c, pl.ds(first, 2 * BLOCK), owner_lanes(k)]

    def to_pair(c, i, k):
        rows = slot_rows(c, k, xl)
        send(("x", c, i), rows, rows, x_s.at[c, i], x_r.at[c, i], pair)

    def finish_reduce(c):
        total = owner_rows(c, z)[...]
        for d in range(2):
            for s in (3, 4) if c in TREES else (ring_steps(c % 2)[d],):
                copies["r", c, d, s].wait()
                total = total + sums[c, d, s - 1]
        mine = slot_rows(c, z, xl)
        mine[...] = total
        if c in SIDEWAYS:
            for d in range(2):
                gather_send(c, d, 1)
        to_pair(c, 0, z)

    def gather_block(c, d, distance):
        return lax.rem(z - (1 - 2 * d) * distance + ROWS, ROWS)

    def gather_copy(c, d, s, distance, hops):
        k = gather_block(c, d, distance)
        rows = slot_rows(c, k, xl) if c in SIDEWAYS else both_sides(c, k)
        send(
            ("a", c, d, s), rows, rows, ag_s.at[c, d, s - 1], ag_r.at[c, d, s - 1],
            at_row((1 - 2 * d) * hops),
        )

    def gather_send(c, d, s):
        steps = ring_steps(1 - c % 2)[d]
        if c not in SPREADS:
            if s <= steps:
                gather_copy(c, d, s, s - 1, 1)
        elif s == 1:
            gather_copy(c, d, 1, 0, 1)
            gather_copy(c, d, 2, 0, 2)
        elif s == 3:
            gather_copy(c, d, 3, 2, 1)
            if steps == 4:
                gather_copy(c, d, 4, 2, 2)

    def gather_step(c, d, s):
        if s == 1:
            copies["x", c, 0].wait()
        else:
            copies["a", c, d, s - 1].wait()
        gather_send(c, d, s)
        if c in SIDEWAYS:
            to_pair(c, 1 + d * ring_steps(1 - c % 2)[0] + s - 2, gather_block(c, d, s - 1))

    def slots_done(c):
        for d in range(2):
            for s in range(ring_steps(1 - c % 2)[d]):
                copies["a", c, d, s + 1].wait()
        for i in range(8 if c in SIDEWAYS else 1):
            copies["x", c, i].wait()

    def project(c, piece, *rows):
        e = CHUNKS[c][0]
        first, number = PIECES[piece]
        slots_done(c)
        weights_done(e, piece)
        top, span = rows[0] * 2 * BLOCK, len(rows) * 2 * BLOCK
        for b in range(first, first + number):
            total = jnp.dot(
                slots[c, top : top + span, :], wbuf[b, e], preferred_element_type=jnp.float32
            )
            for i, row in enumerate(rows):
                for side in range(2):
                    at = (i * 2 + side) * BLOCK
                    part[c, row, b, side] = total[at : at + BLOCK]
        if 0 in rows:
            here = pl.ds(first, number)
            send(
                ("c", c, piece), part.at[c, 0, here], from_core.at[c, here],
                c_s.at[c, piece], c_r.at[c, piece], other_core,
            )

    def to_hi(c, piece):
        e = CHUNKS[c][0]
        first, number = PIECES[piece]
        copies["c", c, piece].wait()

        for b in range(first, first + number):
            for side in range(2):
                part[c, 1, b, side] = part[c, 1, b, side] + from_core[c, b, side]

        here = pl.ds(first, number)
        send(
            ("h", e, piece), part.at[c, 1, here], from_hi.at[e, here],
            h_s.at[e, piece], h_r.at[e, piece], other_hi,
        )

    def hidden(e, side, b):
        c = CHUNKS.index((e, 1))
        total = part[c, 1, b, side] + from_core[c, b, side] + from_hi[e, b, side]
        gate, up = total[:, :LANES], total[:, LANES:]
        return (gate / (1.0 + jnp.exp(-gate)) * up).astype(jnp.bfloat16)

    def positions(piece):
        first, number = PIECES[piece]
        return range(first, first + number), pl.ds(first * LANES, number * LANES)

    def finish_out(e, piece):
        copies["h", e, piece].wait()
        copies["c", CHUNKS.index((e, 1)), piece].wait()
        blocks, lanes = positions(piece)
        for b in blocks:
            sent[e, :, b * LANES : (b + 1) * LANES] = hidden(e, 1 - xl, b)
        send(
            ("o", e, piece), sent.at[e, :, lanes], back.at[e, :, lanes],
            o_s.at[e, piece], o_r.at[e, piece], pair,
        )

    def finish_own(e, piece):
        for b in positions(piece)[0]:
            out_ref[e, :, out_lanes(xl, b)] = hidden(e, xl, b)

    def out_lanes(side, b):
        return pl.ds(pl.multiple_of((side * 4 + lax.rem(y + Y_STEP[b], 4)) * LANES, LANES), LANES)

    def take_back(e, piece):
        copies["o", e, piece].wait()
        for b in positions(piece)[0]:
            out_ref[e, :, out_lanes(1 - xl, b)] = back[e, :, b * LANES : (b + 1) * LANES]

    ids_in.wait()
    find_ranks()
    tok_in.wait()
    for c in range(len(CHUNKS)):
        place_rows(c)
    for e in range(EXPERTS):
        for copy in w_in[e]:
            copy.wait()
    pl.semaphore_wait(barrier, len(partners))
    acts = {
        "w": send_weights, "f": pass_weights, "r": reduce_step, "t": finish_reduce, "a": gather_step,
        "p": project, "h": to_hi, "o": finish_out, "m": finish_own, "b": take_back,
    }
    for step in PLAN:
        acts[step[0]](*map(int, step[1:]))
    for copy in copies.values():
        copy.copy.wait_send()


def shards(tokens, expert_ids, w_gate, w_up):
    bf16, f32 = jnp.bfloat16, jnp.float32
    vmem, dma = pltpu.VMEM, pltpu.SemaphoreType.DMA
    chunks = len(CHUNKS)
    return pl.pallas_call(
        kernel,
        name="experts",
        out_shape=jax.ShapeDtypeStruct((EXPERTS, BLOCK, 1024), bf16),
        in_specs=[pl.BlockSpec(memory_space=pl.ANY)] * 4,
        out_specs=pl.BlockSpec(memory_space=pltpu.VMEM),
        scratch_shapes=[
            vmem(expert_ids.shape[::-1], jnp.int32),
            vmem(tokens.shape, bf16),
            vmem((4, EXPERTS, DEPTH, 2 * LANES), bf16),
            vmem((chunks, 2 * BLOCK, DEPTH), bf16),
            vmem((chunks, 2, 4, BLOCK, QUARTER), bf16),
            vmem((chunks, 4 * BLOCK, DEPTH), bf16),
            vmem((chunks, 2, 4, 2, BLOCK, 2 * LANES), f32),
            vmem((chunks, 4, 2, BLOCK, 2 * LANES), f32),
            vmem((EXPERTS, 4, 2, BLOCK, 2 * LANES), f32),
            vmem((EXPERTS, BLOCK, 4 * LANES), bf16),
            vmem((EXPERTS, BLOCK, 4 * LANES), bf16),
            dma((6,)),
            dma((EXPERTS, 2, 2)), dma((EXPERTS, 2, 2)),
            dma((EXPERTS, 2)), dma((EXPERTS, 2)),
            dma((chunks, 2, 4)), dma((chunks, 2, 4)),
            dma((chunks, 8)), dma((chunks, 8)),
            dma((chunks, 2, 4)), dma((chunks, 2, 4)),
            dma((chunks, 3)), dma((chunks, 3)),
            dma((EXPERTS, 3)), dma((EXPERTS, 3)),
            dma((EXPERTS, 3)), dma((EXPERTS, 3)),
        ],
        compiler_params=pltpu.CompilerParams(
            collective_id=0, has_side_effects=True, vmem_limit_bytes=60 * 1024 * 1024
        ),
    )(expert_ids.T, tokens, w_gate, w_up)


def solution(mesh):
    in_specs = (
        P("row", "layer"),
        P(),
        P(None, "layer", ("row", "col")),
        P(None, "layer", ("row", "col")),
    )
    out_specs = P(None, ("col", "layer"), "row")
    return jax.shard_map(shards, mesh=mesh, in_specs=in_specs, out_specs=out_specs, check_vma=False)
```

```python
import jax
import jax.numpy as jnp
from jax import lax
from jax.experimental import pallas as pl
from jax.experimental.pallas import tpu as pltpu
from jax.sharding import PartitionSpec as P

MESH = pl.DeviceIdType.MESH
ROWS = 8
BLOCK = 80
DEPTH = 1536
QUARTER = DEPTH // 4
HALF = DEPTH // 2
LANES = 128
EXPERTS = 2
CHUNKS = ((0, 0), (1, 0), (0, 1), (1, 1))
TREES = ()
SPREADS = ()
SIDEWAYS = (0,)
Y_STEP = (0, 1, 3, 2)
PIECES = ((0, 1), (1, 2), (3, 1))

PLAN = (
    "w00", "r001", "r211", "r111", "r301", "w01", "r011", "r002", "r212", "r101", "r112", "r302",
    "r012", "r003", "r311", "w10", "r102", "r113", "r201", "r013", "f01", "r004", "f00", "r312",
    "r103", "r114", "r202", "t0", "r313", "r303", "t1", "r203", "w11", "a012", "a002", "r314",
    "a101", "r213", "r204", "a013", "a111", "t3", "a003", "a102", "a014", "t2", "a311", "a301",
    "f10", "f11", "a004", "a112", "a015", "q000", "q010", "a103", "a211", "a201", "k000", "k010",
    "a312", "a302", "q001", "q011", "k001", "a113", "k011", "a104", "q020", "q021", "k020", "k021",
    "a212", "a202", "a313", "a303", "p1001", "p1101", "h10", "a213", "a203", "h11", "a304", "a214",
    "p1201", "p310", "p3001", "p311", "p3201", "h12", "p2101", "p200", "p2201", "p201", "o10", "m10",
    "o01", "m01", "o11", "o00", "m00", "m11", "o02", "m02", "b10", "o12", "m12", "b01",
    "b11", "b00", "b02", "b12",
)


def ring_steps(odd):
    return (3, 4) if odd else (4, 3)


class Copy:
    def __init__(self, src, dst, send_sem, recv_sem, device):
        self.copy = pltpu.make_async_remote_copy(
            src_ref=src, dst_ref=dst, send_sem=send_sem, recv_sem=recv_sem,
            device_id=device, device_id_type=MESH,
        )
        self.copy.start()
        self.arrived = False

    def wait(self):
        if not self.arrived:
            self.copy.wait_recv()
        self.arrived = True


def kernel(
    ids_ref, tok_hbm, wg_hbm, wu_hbm, out_ref,
    tok_ref, wbuf, placed, sums, slots, part, from_core, from_hi, sent, back,
    in_s, w_s, w_r, wf_s, wf_r, rs_s, rs_r, x_s, x_r, ag_s, ag_r, c_s, c_r, h_s, h_r, o_s, o_r,
):
    z = lax.axis_index("row")
    col = lax.axis_index("col")
    layer = lax.axis_index("layer")
    xl, y = col // 4, col % 4
    xh, core = layer // 2, layer % 2

    def at_row(step):
        return (lax.rem(z + step + ROWS, ROWS), col, layer)

    def at_y(step):
        return (z, xl * 4 + lax.rem(y + step, 4), layer)

    pair = (z, (1 - xl) * 4 + y, layer)
    other_core = (z, col, xh * 2 + (1 - core))
    other_hi = (z, col, (1 - xh) * 2 + core)

    barrier = pltpu.get_barrier_semaphore()
    rows_met = (1, -1, 2, -2) if TREES or SPREADS else (1, -1)
    partners = [*map(at_row, rows_met), at_y(1), at_y(3), pair, other_core, other_hi]
    for partner in partners:
        pl.semaphore_signal(barrier, inc=1, device_id=partner, device_id_type=MESH)

    tok_in = pltpu.make_async_copy(tok_hbm, tok_ref, in_s.at[0])
    w_in = [
        [
            pltpu.make_async_copy(
                ref.at[e], wbuf.at[0, e, :, pl.ds(g * LANES, LANES)], in_s.at[1 + 2 * e + g]
            )
            for g, ref in enumerate((wg_hbm, wu_hbm))
        ]
        for e in range(EXPERTS)
    ]
    for copy in (*w_in[1], tok_in, *w_in[0]):
        copy.start()
    here = set()

    def once(*what):
        if what in here:
            return False
        here.add(what)
        return True

    copies = {}

    def send(key, src, dst, send_sem, recv_sem, device):
        copies[key] = Copy(src, dst, send_sem, recv_sem, device)

    def send_weights(e, i):
        if once("w", e):
            for copy in w_in[e]:
                copy.wait()
        for d in range(2):
            half = i if d == 0 else 1 - i
            rows = pl.ds(half * HALF, HALF)
            send(
                ("w", e, d, half), wbuf.at[0, e, rows, :], wbuf.at[2 - d, e, rows, :],
                w_s.at[e, d, half], w_r.at[e, d, half], at_y(1 if d == 0 else 3),
            )

    def pass_weights(e, d):
        copies["w", e, d, d].wait()
        rows = pl.ds(d * HALF, HALF)
        send(
            ("f", e, d), wbuf.at[2 - d, e, rows, :], wbuf.at[3, e, rows, :],
            wf_s.at[e, d], wf_r.at[e, d], at_y(1 if d == 0 else 3),
        )

    def weights_done(e, piece):
        if piece == 1:
            for d in range(2):
                for half in range(2):
                    copies["w", e, d, half].wait()
        elif piece == 2:
            for d in range(2):
                copies["f", e, d].wait()

    count = tok_ref.shape[0]
    start = pl.multiple_of(z * count, LANES)
    rank = []

    def find_ranks():
        above = lax.broadcasted_iota(jnp.int32, (count, count), 0)
        right = lax.broadcasted_iota(jnp.int32, (count, count), 1)
        before = (above < right).astype(jnp.float32).astype(jnp.bfloat16)
        token = lax.broadcasted_iota(jnp.int32, (1, ids_ref.shape[1]), 1)
        for e in range(EXPERTS):
            named = (ids_ref[0:1, :] == e) | (ids_ref[1:2, :] == e)
            ahead = jnp.sum((named & (token < start)).astype(jnp.float32), axis=1, keepdims=True)
            lanes = pl.ds(start, count)
            own = (ids_ref[0:1, lanes] == e) | (ids_ref[1:2, lanes] == e)
            ones = jnp.broadcast_to(own.astype(jnp.float32), (16, count)).astype(jnp.bfloat16)
            within = jnp.dot(ones, before, preferred_element_type=jnp.float32)[0:1]
            rank.append(jnp.where(own, (within + ahead).astype(jnp.int32), -1))

    def slot_start(c, r):
        to_hi = xh if CHUNKS[c][1] else 1 - xh
        to_core = core if r else 1 - core
        return (col * 4 + to_hi * 2 + to_core) * BLOCK

    def place_rows(c):
        if once("ids"):
            find_ranks()
            tok_in.wait()
        index = lax.broadcasted_iota(jnp.int32, (BLOCK, count), 0)
        slot = jnp.concatenate([index + slot_start(c, 0), index + slot_start(c, 1)], axis=0)
        pick = (slot == rank[CHUNKS[c][0]]).astype(jnp.float32).astype(jnp.bfloat16)
        for f in range(2):
            placed[c, :, f * HALF : (f + 1) * HALF] = jnp.dot(
                pick, tok_ref[:, f * HALF : (f + 1) * HALF], preferred_element_type=jnp.float32
            ).astype(jnp.bfloat16)

    def owner_lanes(k):
        return pl.ds(pl.multiple_of((k % 4) * QUARTER, LANES), QUARTER)

    def owner_rows(c, k):
        return placed.at[c, pl.ds(pl.multiple_of((k // 4) * BLOCK, 16), BLOCK), owner_lanes(k)]

    def reduce_send(c, d, s, src, hops):
        send(
            ("r", c, d, s), src, sums.at[c, d, s - 1],
            rs_s.at[c, d, s - 1], rs_r.at[c, d, s - 1], at_row((1 - 2 * d) * hops),
        )

    def reduce_step(c, d, s):
        sign, steps = 1 - 2 * d, ring_steps(c % 2)[d]
        if once("p", c):
            place_rows(c)

        def rows_for(distance):
            return owner_rows(c, lax.rem(z + sign * distance + ROWS, ROWS))

        if c not in TREES:
            src = rows_for(steps - s + 1)
            if s > 1:
                copies["r", c, d, s - 1].wait()
                sums[c, d, s - 2] = sums[c, d, s - 2] + src[...]
                src = sums.at[c, d, s - 2]
            reduce_send(c, d, s, src, 1)
        elif s == 1:
            reduce_send(c, d, 1, rows_for(3), 1)
            if steps == 4:
                reduce_send(c, d, 2, rows_for(4), 2)
            reduce_send(c, d, 4, rows_for(1), 1)
        else:
            copies["r", c, d, 1].wait()
            total = sums[c, d, 0] + rows_for(2)[...]
            if steps == 4:
                copies["r", c, d, 2].wait()
                total = total + sums[c, d, 1]
            sums[c, d, 0] = total
            reduce_send(c, d, 3, sums.at[c, d, 0], 2)

    def slot_rows(c, k, side):
        first = pl.multiple_of((k // 4) * (2 * BLOCK) + side * BLOCK, 16)
        return slots.at[c, pl.ds(first, BLOCK), owner_lanes(k)]

    def both_sides(c, k):
        first = pl.multiple_of((k // 4) * (2 * BLOCK), 16)
        return slots.at[c, pl.ds(first, 2 * BLOCK), owner_lanes(k)]

    def to_pair(c, i, k):
        rows = slot_rows(c, k, xl)
        send(("x", c, i), rows, rows, x_s.at[c, i], x_r.at[c, i], pair)

    def finish_reduce(c):
        total = owner_rows(c, z)[...]
        for d in range(2):
            for s in (3, 4) if c in TREES else (ring_steps(c % 2)[d],):
                copies["r", c, d, s].wait()
                total = total + sums[c, d, s - 1]
        mine = slot_rows(c, z, xl)
        mine[...] = total
        if c in SIDEWAYS:
            for d in range(2):
                gather_send(c, d, 1)
        to_pair(c, 0, z)

    def gather_block(c, d, distance):
        return lax.rem(z - (1 - 2 * d) * distance + ROWS, ROWS)

    def gather_copy(c, d, s, distance, hops):
        k = gather_block(c, d, distance)
        rows = slot_rows(c, k, xl) if c in SIDEWAYS else both_sides(c, k)
        send(
            ("a", c, d, s), rows, rows, ag_s.at[c, d, s - 1], ag_r.at[c, d, s - 1],
            at_row((1 - 2 * d) * hops),
        )

    def gather_send(c, d, s):
        steps = ring_steps(1 - c % 2)[d]
        if c not in SPREADS:
            if s <= steps:
                gather_copy(c, d, s, s - 1, 1)
        elif s == 1:
            gather_copy(c, d, 1, 0, 1)
            gather_copy(c, d, 2, 0, 2)
        elif s == 3:
            gather_copy(c, d, 3, 2, 1)
            if steps == 4:
                gather_copy(c, d, 4, 2, 2)

    def gather_step(c, d, s):
        if s == 1:
            copies["x", c, 0].wait()
        else:
            copies["a", c, d, s - 1].wait()
        gather_send(c, d, s)
        if c in SIDEWAYS:
            to_pair(c, 1 + d * ring_steps(1 - c % 2)[0] + s - 2, gather_block(c, d, s - 1))

    def slots_done(c, own_only=False):
        for d in range(2):
            for s in range(ring_steps(1 - c % 2)[d]):
                copies["a", c, d, s + 1].wait()
        if not own_only:
            for i in range(8 if c in SIDEWAYS else 1):
                copies["x", c, i].wait()

    def project_side(c, piece, s):
        e = CHUNKS[c][0]
        first, number = PIECES[piece]
        side = xl if s == 0 else 1 - xl
        slots_done(c, s == 0)
        weights_done(e, piece)
        low = pl.multiple_of(side * BLOCK, 16)
        rows = jnp.concatenate(
            [slots[c, pl.ds(low, BLOCK), :], slots[c, pl.ds(low + 2 * BLOCK, BLOCK), :]], axis=0
        )
        for b in range(first, first + number):
            total = jnp.dot(rows, wbuf[b, e], preferred_element_type=jnp.float32)
            for r in range(2):
                part[c, r, b, side] = total[r * BLOCK : (r + 1) * BLOCK]
        span = pl.ds(first, number)
        send(
            ("c", c, piece, s), part.at[c, 0, span, side], from_core.at[c, span, side],
            c_s.at[c, piece, s], c_r.at[c, piece, s], other_core,
        )

    def to_hi_side(c, piece, s):
        e = CHUNKS[c][0]
        first, number = PIECES[piece]
        side = xl if s == 0 else 1 - xl
        copies["c", c, piece, s].wait()
        for b in range(first, first + number):
            part[c, 1, b, side] = part[c, 1, b, side] + from_core[c, b, side]
        span = pl.ds(first, number)
        send(
            ("h", e, piece, s), part.at[c, 1, span, side], from_hi.at[e, span, side],
            h_s.at[e, piece, s], h_r.at[e, piece, s], other_hi,
        )

    def project(c, piece, *rows):
        e = CHUNKS[c][0]
        first, number = PIECES[piece]
        slots_done(c)
        weights_done(e, piece)
        top, span = rows[0] * 2 * BLOCK, len(rows) * 2 * BLOCK
        for b in range(first, first + number):
            total = jnp.dot(
                slots[c, top : top + span, :], wbuf[b, e], preferred_element_type=jnp.float32
            )
            for i, row in enumerate(rows):
                for side in range(2):
                    at = (i * 2 + side) * BLOCK
                    part[c, row, b, side] = total[at : at + BLOCK]
        if 0 in rows:
            span = pl.ds(first, number)
            send(
                ("c", c, piece, 0), part.at[c, 0, span], from_core.at[c, span],
                c_s.at[c, piece, 0], c_r.at[c, piece, 0], other_core,
            )

    def to_hi(c, piece):
        e = CHUNKS[c][0]
        first, number = PIECES[piece]
        copies["c", c, piece, 0].wait()

        for b in range(first, first + number):
            for side in range(2):
                part[c, 1, b, side] = part[c, 1, b, side] + from_core[c, b, side]

        span = pl.ds(first, number)
        send(
            ("h", e, piece, 0), part.at[c, 1, span], from_hi.at[e, span],
            h_s.at[e, piece, 0], h_r.at[e, piece, 0], other_hi,
        )

    def hidden(e, side, b):
        c = CHUNKS.index((e, 1))
        total = part[c, 1, b, side] + from_core[c, b, side] + from_hi[e, b, side]
        gate, up = total[:, :LANES], total[:, LANES:]
        return (gate / (1.0 + jnp.exp(-gate)) * up).astype(jnp.bfloat16)

    def positions(piece):
        first, number = PIECES[piece]
        return range(first, first + number), pl.ds(first * LANES, number * LANES)

    def finish_out(e, piece):
        for s in range(2 if CHUNKS.index((e, 0)) in SIDEWAYS else 1):
            copies["h", e, piece, s].wait()
        copies["c", CHUNKS.index((e, 1)), piece, 0].wait()
        blocks, lanes = positions(piece)
        for b in blocks:
            sent[e, :, b * LANES : (b + 1) * LANES] = hidden(e, 1 - xl, b)
        send(
            ("o", e, piece), sent.at[e, :, lanes], back.at[e, :, lanes],
            o_s.at[e, piece], o_r.at[e, piece], pair,
        )

    def finish_own(e, piece):
        for b in positions(piece)[0]:
            out_ref[e, :, out_lanes(xl, b)] = hidden(e, xl, b)

    def out_lanes(side, b):
        return pl.ds(pl.multiple_of((side * 4 + lax.rem(y + Y_STEP[b], 4)) * LANES, LANES), LANES)

    def take_back(e, piece):
        copies["o", e, piece].wait()
        for b in positions(piece)[0]:
            out_ref[e, :, out_lanes(1 - xl, b)] = back[e, :, b * LANES : (b + 1) * LANES]

    pl.semaphore_wait(barrier, len(partners))
    acts = {
        "w": send_weights, "f": pass_weights, "r": reduce_step, "t": finish_reduce, "a": gather_step,
        "p": project, "h": to_hi, "q": project_side, "k": to_hi_side, "o": finish_out, "m": finish_own, "b": take_back,
    }
    for step in PLAN:
        acts[step[0]](*map(int, step[1:]))
    for copy in copies.values():
        copy.copy.wait_send()


def shards(tokens, expert_ids, w_gate, w_up):
    bf16, f32 = jnp.bfloat16, jnp.float32
    vmem, dma = pltpu.VMEM, pltpu.SemaphoreType.DMA
    chunks = len(CHUNKS)
    return pl.pallas_call(
        kernel,
        name="experts",
        out_shape=jax.ShapeDtypeStruct((EXPERTS, BLOCK, 1024), bf16),
        in_specs=[pl.BlockSpec(memory_space=pltpu.VMEM)] + [pl.BlockSpec(memory_space=pl.ANY)] * 3,
        out_specs=pl.BlockSpec(memory_space=pltpu.VMEM),
        scratch_shapes=[
            vmem(tokens.shape, bf16),
            vmem((4, EXPERTS, DEPTH, 2 * LANES), bf16),
            vmem((chunks, 2 * BLOCK, DEPTH), bf16),
            vmem((chunks, 2, 4, BLOCK, QUARTER), bf16),
            vmem((chunks, 4 * BLOCK, DEPTH), bf16),
            vmem((chunks, 2, 4, 2, BLOCK, 2 * LANES), f32),
            vmem((chunks, 4, 2, BLOCK, 2 * LANES), f32),
            vmem((EXPERTS, 4, 2, BLOCK, 2 * LANES), f32),
            vmem((EXPERTS, BLOCK, 4 * LANES), bf16),
            vmem((EXPERTS, BLOCK, 4 * LANES), bf16),
            dma((5,)),
            dma((EXPERTS, 2, 2)), dma((EXPERTS, 2, 2)),
            dma((EXPERTS, 2)), dma((EXPERTS, 2)),
            dma((chunks, 2, 4)), dma((chunks, 2, 4)),
            dma((chunks, 8)), dma((chunks, 8)),
            dma((chunks, 2, 4)), dma((chunks, 2, 4)),
            dma((chunks, 3, 2)), dma((chunks, 3, 2)),
            dma((EXPERTS, 3, 2)), dma((EXPERTS, 3, 2)),
            dma((EXPERTS, 3)), dma((EXPERTS, 3)),
        ],
        compiler_params=pltpu.CompilerParams(
            collective_id=0, has_side_effects=True, vmem_limit_bytes=55920000
        ),
    )(expert_ids.T, tokens, w_gate, w_up)


def solution(mesh):
    in_specs = (
        P("row", "layer"),
        P(),
        P(None, "layer", ("row", "col")),
        P(None, "layer", ("row", "col")),
    )
    out_specs = P(None, ("col", "layer"), "row")
    return jax.shard_map(shards, mesh=mesh, in_specs=in_specs, out_specs=out_specs, check_vma=False)
```

```python
import jax
import jax.numpy as jnp
from jax import lax
from jax.experimental import pallas as pl
from jax.experimental.pallas import tpu as pltpu
from jax.sharding import PartitionSpec as P

MESH = pl.DeviceIdType.MESH
ROWS = 8
BLOCK = 80
DEPTH = 1536
QUARTER = DEPTH // 4
HALF = DEPTH // 2
LANES = 128
EXPERTS = 2
CHUNKS = ((0, 0), (1, 0), (0, 1), (1, 1))
TREES = ()
SPREADS = ()
SIDEWAYS = (0,)
Y_STEP = (0, 1, 3, 2)
PIECES = ((0, 1), (1, 2), (3, 1))

PLAN = (
    "w00", "r001", "r101", "r111", "r011", "r301", "r211", "w01", "r002", "r112", "r102", "r012",
    "r212", "r003", "r113", "r201", "r311", "r103", "r013", "r004", "w10", "f00", "r114", "r302",
    "r202", "r312", "t0", "t1", "f01", "r303", "r313", "r203", "a012", "r213", "a002", "a101",
    "r314", "w11", "r204", "a013", "a003", "a111", "t3", "a102", "a014", "t2", "f10", "a004",
    "a301", "a311", "a112", "a015", "q010", "q000", "a103", "a211", "a201", "k010", "k000", "a312",
    "a302", "q011", "q001", "k011", "k001", "a113", "a104", "q021", "q020", "f11", "k021", "k020",
    "a212", "a202", "a313", "a303", "p1001", "p1101", "h10", "a213", "a203", "h11", "a304", "a214",
    "p1201", "p310", "p3201", "h12", "p311", "p3001", "p2101", "p2201", "p2001", "o10", "m10", "o01",
    "m01", "o02", "m02", "o11", "m11", "o00", "m00", "b10", "o12", "m12", "b01", "b02",
    "b11", "b00", "b12",
)


def ring_steps(odd):
    return (3, 4) if odd else (4, 3)


class Copy:
    def __init__(self, src, dst, send_sem, recv_sem, device):
        self.copy = pltpu.make_async_remote_copy(
            src_ref=src, dst_ref=dst, send_sem=send_sem, recv_sem=recv_sem,
            device_id=device, device_id_type=MESH,
        )
        self.copy.start()
        self.arrived = False

    def wait(self):
        if not self.arrived:
            self.copy.wait_recv()
        self.arrived = True


def kernel(
    ids_ref, tok_hbm, wg_hbm, wu_hbm, out_ref,
    tok_ref, wbuf, placed, sums, slots, part, from_core, from_hi, sent, back,
    in_s, w_s, w_r, wf_s, wf_r, rs_s, rs_r, x_s, x_r, ag_s, ag_r, c_s, c_r, h_s, h_r, o_s, o_r,
):
    z = lax.axis_index("row")
    col = lax.axis_index("col")
    layer = lax.axis_index("layer")
    xl, y = col // 4, col % 4
    xh, core = layer // 2, layer % 2

    def at_row(step):
        return (lax.rem(z + step + ROWS, ROWS), col, layer)

    def at_y(step):
        return (z, xl * 4 + lax.rem(y + step, 4), layer)

    pair = (z, (1 - xl) * 4 + y, layer)
    other_core = (z, col, xh * 2 + (1 - core))
    other_hi = (z, col, (1 - xh) * 2 + core)

    barrier = pltpu.get_barrier_semaphore()
    rows_met = (1, -1, 2, -2) if TREES or SPREADS else (1, -1)
    partners = [*map(at_row, rows_met), at_y(1), at_y(3), pair, other_core, other_hi]
    for partner in partners:
        pl.semaphore_signal(barrier, inc=1, device_id=partner, device_id_type=MESH)

    tok_in = pltpu.make_async_copy(tok_hbm, tok_ref, in_s.at[0])
    w_in = [
        [
            pltpu.make_async_copy(
                ref.at[e], wbuf.at[0, e, :, pl.ds(g * LANES, LANES)], in_s.at[1 + 2 * e + g]
            )
            for g, ref in enumerate((wg_hbm, wu_hbm))
        ]
        for e in range(EXPERTS)
    ]
    for copy in (*w_in[1], tok_in, *w_in[0]):
        copy.start()
    here = set()

    def once(*what):
        if what in here:
            return False
        here.add(what)
        return True

    copies = {}

    def send(key, src, dst, send_sem, recv_sem, device):
        copies[key] = Copy(src, dst, send_sem, recv_sem, device)

    def send_weights(e, i):
        if once("w", e):
            for copy in w_in[e]:
                copy.wait()
        for d in range(2):
            half = i if d == 0 else 1 - i
            rows = pl.ds(half * HALF, HALF)
            send(
                ("w", e, d, half), wbuf.at[0, e, rows, :], wbuf.at[2 - d, e, rows, :],
                w_s.at[e, d, half], w_r.at[e, d, half], at_y(1 if d == 0 else 3),
            )

    def pass_weights(e, d):
        copies["w", e, d, d].wait()
        rows = pl.ds(d * HALF, HALF)
        send(
            ("f", e, d), wbuf.at[2 - d, e, rows, :], wbuf.at[3, e, rows, :],
            wf_s.at[e, d], wf_r.at[e, d], at_y(1 if d == 0 else 3),
        )

    def weights_done(e, piece):
        if piece == 1:
            for d in range(2):
                for half in range(2):
                    copies["w", e, d, half].wait()
        elif piece == 2:
            for d in range(2):
                copies["f", e, d].wait()

    count = tok_ref.shape[0]
    start = pl.multiple_of(z * count, LANES)
    rank = []

    def find_ranks():
        above = lax.broadcasted_iota(jnp.int32, (count, count), 0)
        right = lax.broadcasted_iota(jnp.int32, (count, count), 1)
        before = (above < right).astype(jnp.float32).astype(jnp.bfloat16)
        token = lax.broadcasted_iota(jnp.int32, (1, ids_ref.shape[1]), 1)
        for e in range(EXPERTS):
            named = (ids_ref[0:1, :] == e) | (ids_ref[1:2, :] == e)
            ahead = jnp.sum((named & (token < start)).astype(jnp.float32), axis=1, keepdims=True)
            lanes = pl.ds(start, count)
            own = (ids_ref[0:1, lanes] == e) | (ids_ref[1:2, lanes] == e)
            ones = jnp.broadcast_to(own.astype(jnp.float32), (16, count)).astype(jnp.bfloat16)
            within = jnp.dot(ones, before, preferred_element_type=jnp.float32)[0:1]
            rank.append(jnp.where(own, (within + ahead).astype(jnp.int32), -1))

    def slot_start(c, r):
        to_hi = xh if CHUNKS[c][1] else 1 - xh
        to_core = core if r else 1 - core
        return (col * 4 + to_hi * 2 + to_core) * BLOCK

    def place_rows(c):
        if once("tok"):
            tok_in.wait()
        index = lax.broadcasted_iota(jnp.int32, (BLOCK, count), 0)
        slot = jnp.concatenate([index + slot_start(c, 0), index + slot_start(c, 1)], axis=0)
        pick = (slot == rank[CHUNKS[c][0]]).astype(jnp.float32).astype(jnp.bfloat16)
        for f in range(2):
            placed[c, :, f * HALF : (f + 1) * HALF] = jnp.dot(
                pick, tok_ref[:, f * HALF : (f + 1) * HALF], preferred_element_type=jnp.float32
            ).astype(jnp.bfloat16)

    def owner_lanes(k):
        return pl.ds(pl.multiple_of((k % 4) * QUARTER, LANES), QUARTER)

    def owner_rows(c, k):
        return placed.at[c, pl.ds(pl.multiple_of((k // 4) * BLOCK, 16), BLOCK), owner_lanes(k)]

    def reduce_send(c, d, s, src, hops):
        send(
            ("r", c, d, s), src, sums.at[c, d, s - 1],
            rs_s.at[c, d, s - 1], rs_r.at[c, d, s - 1], at_row((1 - 2 * d) * hops),
        )

    def reduce_step(c, d, s):
        sign, steps = 1 - 2 * d, ring_steps(c % 2)[d]
        if once("p", c):
            place_rows(c)

        def rows_for(distance):
            return owner_rows(c, lax.rem(z + sign * distance + ROWS, ROWS))

        if c not in TREES:
            src = rows_for(steps - s + 1)
            if s > 1:
                copies["r", c, d, s - 1].wait()
                sums[c, d, s - 2] = sums[c, d, s - 2] + src[...]
                src = sums.at[c, d, s - 2]
            reduce_send(c, d, s, src, 1)
        elif s == 1:
            reduce_send(c, d, 1, rows_for(3), 1)
            if steps == 4:
                reduce_send(c, d, 2, rows_for(4), 2)
            reduce_send(c, d, 4, rows_for(1), 1)
        else:
            copies["r", c, d, 1].wait()
            total = sums[c, d, 0] + rows_for(2)[...]
            if steps == 4:
                copies["r", c, d, 2].wait()
                total = total + sums[c, d, 1]
            sums[c, d, 0] = total
            reduce_send(c, d, 3, sums.at[c, d, 0], 2)

    def slot_rows(c, k, side):
        first = pl.multiple_of((k // 4) * (2 * BLOCK) + side * BLOCK, 16)
        return slots.at[c, pl.ds(first, BLOCK), owner_lanes(k)]

    def both_sides(c, k):
        first = pl.multiple_of((k // 4) * (2 * BLOCK), 16)
        return slots.at[c, pl.ds(first, 2 * BLOCK), owner_lanes(k)]

    def to_pair(c, i, k):
        rows = slot_rows(c, k, xl)
        send(("x", c, i), rows, rows, x_s.at[c, i], x_r.at[c, i], pair)

    def finish_reduce(c):
        total = owner_rows(c, z)[...]
        for d in range(2):
            for s in (3, 4) if c in TREES else (ring_steps(c % 2)[d],):
                copies["r", c, d, s].wait()
                total = total + sums[c, d, s - 1]
        mine = slot_rows(c, z, xl)
        mine[...] = total
        if c in SIDEWAYS:
            for d in range(2):
                gather_send(c, d, 1)
        to_pair(c, 0, z)

    def gather_block(c, d, distance):
        return lax.rem(z - (1 - 2 * d) * distance + ROWS, ROWS)

    def gather_copy(c, d, s, distance, hops):
        k = gather_block(c, d, distance)
        rows = slot_rows(c, k, xl) if c in SIDEWAYS else both_sides(c, k)
        send(
            ("a", c, d, s), rows, rows, ag_s.at[c, d, s - 1], ag_r.at[c, d, s - 1],
            at_row((1 - 2 * d) * hops),
        )

    def gather_send(c, d, s):
        steps = ring_steps(1 - c % 2)[d]
        if c not in SPREADS:
            if s <= steps:
                gather_copy(c, d, s, s - 1, 1)
        elif s == 1:
            gather_copy(c, d, 1, 0, 1)
            gather_copy(c, d, 2, 0, 2)
        elif s == 3:
            gather_copy(c, d, 3, 2, 1)
            if steps == 4:
                gather_copy(c, d, 4, 2, 2)

    def gather_step(c, d, s):
        if s == 1:
            copies["x", c, 0].wait()
        else:
            copies["a", c, d, s - 1].wait()
        gather_send(c, d, s)
        if c in SIDEWAYS:
            to_pair(c, 1 + d * ring_steps(1 - c % 2)[0] + s - 2, gather_block(c, d, s - 1))

    def slots_done(c, own_only=False):
        for d in range(2):
            for s in range(ring_steps(1 - c % 2)[d]):
                copies["a", c, d, s + 1].wait()
        if not own_only:
            for i in range(8 if c in SIDEWAYS else 1):
                copies["x", c, i].wait()

    def project_side(c, piece, s):
        e = CHUNKS[c][0]
        first, number = PIECES[piece]
        side = xl if s == 0 else 1 - xl
        slots_done(c, s == 0)
        weights_done(e, piece)
        low = pl.multiple_of(side * BLOCK, 16)
        rows = jnp.concatenate(
            [slots[c, pl.ds(low, BLOCK), :], slots[c, pl.ds(low + 2 * BLOCK, BLOCK), :]], axis=0
        )
        for b in range(first, first + number):
            total = jnp.dot(rows, wbuf[b, e], preferred_element_type=jnp.float32)
            for r in range(2):
                part[c, r, b, side] = total[r * BLOCK : (r + 1) * BLOCK]
        span = pl.ds(first, number)
        send(
            ("c", c, piece, s), part.at[c, 0, span, side], from_core.at[c, span, side],
            c_s.at[c, piece, s], c_r.at[c, piece, s], other_core,
        )

    def to_hi_side(c, piece, s):
        e = CHUNKS[c][0]
        first, number = PIECES[piece]
        side = xl if s == 0 else 1 - xl
        copies["c", c, piece, s].wait()
        for b in range(first, first + number):
            part[c, 1, b, side] = part[c, 1, b, side] + from_core[c, b, side]
        span = pl.ds(first, number)
        send(
            ("h", e, piece, s), part.at[c, 1, span, side], from_hi.at[e, span, side],
            h_s.at[e, piece, s], h_r.at[e, piece, s], other_hi,
        )

    def project(c, piece, *rows):
        e = CHUNKS[c][0]
        first, number = PIECES[piece]
        slots_done(c)
        weights_done(e, piece)
        top, span = rows[0] * 2 * BLOCK, len(rows) * 2 * BLOCK
        for b in range(first, first + number):
            total = jnp.dot(
                slots[c, top : top + span, :], wbuf[b, e], preferred_element_type=jnp.float32
            )
            for i, row in enumerate(rows):
                for side in range(2):
                    at = (i * 2 + side) * BLOCK
                    part[c, row, b, side] = total[at : at + BLOCK]
        if 0 in rows:
            span = pl.ds(first, number)
            send(
                ("c", c, piece, 0), part.at[c, 0, span], from_core.at[c, span],
                c_s.at[c, piece, 0], c_r.at[c, piece, 0], other_core,
            )

    def to_hi(c, piece):
        e = CHUNKS[c][0]
        first, number = PIECES[piece]
        copies["c", c, piece, 0].wait()

        for b in range(first, first + number):
            for side in range(2):
                part[c, 1, b, side] = part[c, 1, b, side] + from_core[c, b, side]

        span = pl.ds(first, number)
        send(
            ("h", e, piece, 0), part.at[c, 1, span], from_hi.at[e, span],
            h_s.at[e, piece, 0], h_r.at[e, piece, 0], other_hi,
        )

    def hidden(e, side, b):
        c = CHUNKS.index((e, 1))
        total = part[c, 1, b, side] + from_core[c, b, side] + from_hi[e, b, side]
        gate, up = total[:, :LANES], total[:, LANES:]
        return (gate / (1.0 + jnp.exp(-gate)) * up).astype(jnp.bfloat16)

    def positions(piece):
        first, number = PIECES[piece]
        return range(first, first + number), pl.ds(first * LANES, number * LANES)

    def finish_out(e, piece):
        for s in range(2 if CHUNKS.index((e, 0)) in SIDEWAYS else 1):
            copies["h", e, piece, s].wait()
        copies["c", CHUNKS.index((e, 1)), piece, 0].wait()
        blocks, lanes = positions(piece)
        for b in blocks:
            sent[e, :, b * LANES : (b + 1) * LANES] = hidden(e, 1 - xl, b)
        send(
            ("o", e, piece), sent.at[e, :, lanes], back.at[e, :, lanes],
            o_s.at[e, piece], o_r.at[e, piece], pair,
        )

    def finish_own(e, piece):
        for b in positions(piece)[0]:
            out_ref[e, :, out_lanes(xl, b)] = hidden(e, xl, b)

    def out_lanes(side, b):
        return pl.ds(pl.multiple_of((side * 4 + lax.rem(y + Y_STEP[b], 4)) * LANES, LANES), LANES)

    def take_back(e, piece):
        copies["o", e, piece].wait()
        for b in positions(piece)[0]:
            out_ref[e, :, out_lanes(1 - xl, b)] = back[e, :, b * LANES : (b + 1) * LANES]

    find_ranks()
    pl.semaphore_wait(barrier, len(partners))
    acts = {
        "w": send_weights, "f": pass_weights, "r": reduce_step, "t": finish_reduce, "a": gather_step,
        "p": project, "h": to_hi, "q": project_side, "k": to_hi_side, "o": finish_out, "m": finish_own, "b": take_back,
    }
    for step in PLAN:
        acts[step[0]](*map(int, step[1:]))
    for copy in copies.values():
        copy.copy.wait_send()


def shards(tokens, expert_ids, w_gate, w_up):
    bf16, f32 = jnp.bfloat16, jnp.float32
    vmem, dma = pltpu.VMEM, pltpu.SemaphoreType.DMA
    chunks = len(CHUNKS)
    return pl.pallas_call(
        kernel,
        name="experts",
        out_shape=jax.ShapeDtypeStruct((EXPERTS, BLOCK, 1024), bf16),
        in_specs=[pl.BlockSpec(memory_space=pltpu.VMEM)] + [pl.BlockSpec(memory_space=pl.ANY)] * 3,
        out_specs=pl.BlockSpec(memory_space=pltpu.VMEM),
        scratch_shapes=[
            vmem(tokens.shape, bf16),
            vmem((4, EXPERTS, DEPTH, 2 * LANES), bf16),
            vmem((chunks, 2 * BLOCK, DEPTH), bf16),
            vmem((chunks, 2, 4, BLOCK, QUARTER), bf16),
            vmem((chunks, 4 * BLOCK, DEPTH), bf16),
            vmem((chunks, 2, 4, 2, BLOCK, 2 * LANES), f32),
            vmem((chunks, 4, 2, BLOCK, 2 * LANES), f32),
            vmem((EXPERTS, 4, 2, BLOCK, 2 * LANES), f32),
            vmem((EXPERTS, BLOCK, 4 * LANES), bf16),
            vmem((EXPERTS, BLOCK, 4 * LANES), bf16),
            dma((5,)),
            dma((EXPERTS, 2, 2)), dma((EXPERTS, 2, 2)),
            dma((EXPERTS, 2)), dma((EXPERTS, 2)),
            dma((chunks, 2, 4)), dma((chunks, 2, 4)),
            dma((chunks, 8)), dma((chunks, 8)),
            dma((chunks, 2, 4)), dma((chunks, 2, 4)),
            dma((chunks, 3, 2)), dma((chunks, 3, 2)),
            dma((EXPERTS, 3, 2)), dma((EXPERTS, 3, 2)),
            dma((EXPERTS, 3)), dma((EXPERTS, 3)),
        ],
        compiler_params=pltpu.CompilerParams(
            collective_id=0, has_side_effects=True, vmem_limit_bytes=55920000
        ),
    )(expert_ids.T, tokens, w_gate, w_up)


def solution(mesh):
    in_specs = (
        P("row", "layer"),
        P(),
        P(None, "layer", ("row", "col")),
        P(None, "layer", ("row", "col")),
    )
    out_specs = P(None, ("col", "layer"), "row")
    return jax.shard_map(shards, mesh=mesh, in_specs=in_specs, out_specs=out_specs, check_vma=False)
```

```python
import jax
import jax.numpy as jnp
from jax import lax
from jax.experimental import pallas as pl
from jax.experimental.pallas import tpu as pltpu
from jax.sharding import PartitionSpec as P

MESH = pl.DeviceIdType.MESH
ROWS = 8
BLOCK = 80
DEPTH = 1536
QUARTER = DEPTH // 4
HALF = DEPTH // 2
LANES = 128
EXPERTS = 2
CHUNKS = ((0, 0), (1, 0), (0, 1), (1, 1))
TREES = ()
SPREADS = ()
SIDEWAYS = (0,)
Y_STEP = (0, 1, 3, 2)
PIECES = ((0, 1), (1, 2), (3, 1))

PLAN = (
    "w00", "r001", "r101", "r111", "r011", "r301", "r211", "w01", "r002", "r112", "r102", "r012",
    "r212", "r003", "r113", "r201", "r311", "r103", "r013", "r004", "w10", "f00", "r114", "r302",
    "r202", "r312", "t0", "t1", "f01", "r303", "r313", "r203", "a012", "r213", "a002", "a101",
    "r314", "w11", "r204", "a013", "a003", "a111", "t3", "a102", "a014", "t2", "f10", "a004",
    "a301", "a311", "a112", "a015", "q010", "q000", "a103", "a211", "a201", "k010", "k000", "a312",
    "a302", "q011", "q001", "k011", "k001", "a113", "a104", "q021", "q020", "f11", "k021", "k020",
    "a212", "a202", "a313", "a303", "p1001", "p1101", "h10", "a213", "a203", "h11", "a304", "a214",
    "p1201", "p310", "p3201", "h12", "p311", "p3001", "p2101", "p2201", "p2001", "o10", "m10", "o01",
    "m01", "o02", "m02", "o11", "m11", "o00", "m00", "b10", "o12", "m12", "b01", "b02",
    "b11", "b00", "b12",
)


def ring_steps(odd):
    return (3, 4) if odd else (4, 3)


class Copy:
    def __init__(self, src, dst, send_sem, recv_sem, device):
        self.copy = pltpu.make_async_remote_copy(
            src_ref=src, dst_ref=dst, send_sem=send_sem, recv_sem=recv_sem,
            device_id=device, device_id_type=MESH,
        )
        self.copy.start()
        self.arrived = False

    def wait(self):
        if not self.arrived:
            self.copy.wait_recv()
        self.arrived = True


def kernel(
    ids_ref, tok_hbm, wg_hbm, wu_hbm, out_ref,
    tok_ref, wbuf, placed, sums, slots, part, from_core, from_hi, sent, back,
    in_s, w_s, w_r, wf_s, wf_r, rs_s, rs_r, x_s, x_r, ag_s, ag_r, c_s, c_r, h_s, h_r, o_s, o_r,
):
    z = lax.axis_index("row")
    col = lax.axis_index("col")
    layer = lax.axis_index("layer")
    xl, y = col // 4, col % 4
    xh, core = layer // 2, layer % 2

    def at_row(step):
        return (lax.rem(z + step + ROWS, ROWS), col, layer)

    def at_y(step):
        return (z, xl * 4 + lax.rem(y + step, 4), layer)

    pair = (z, (1 - xl) * 4 + y, layer)
    other_core = (z, col, xh * 2 + (1 - core))
    other_hi = (z, col, (1 - xh) * 2 + core)

    barrier = pltpu.get_barrier_semaphore()
    rows_met = (1, -1, 2, -2) if TREES or SPREADS else (1, -1)
    partners = [*map(at_row, rows_met), at_y(1), at_y(3), pair, other_core, other_hi]
    for partner in partners:
        pl.semaphore_signal(barrier, inc=1, device_id=partner, device_id_type=MESH)

    tok_in = pltpu.make_async_copy(tok_hbm, tok_ref, in_s.at[0])
    w_in = [
        [
            pltpu.make_async_copy(
                ref.at[e], wbuf.at[0, e, :, pl.ds(g * LANES, LANES)], in_s.at[1 + 2 * e + g]
            )
            for g, ref in enumerate((wg_hbm, wu_hbm))
        ]
        for e in range(EXPERTS)
    ]
    for copy in (*w_in[1], tok_in, *w_in[0]):
        copy.start()
    here = set()

    def once(*what):
        if what in here:
            return False
        here.add(what)
        return True

    copies = {}

    def send(key, src, dst, send_sem, recv_sem, device):
        copies[key] = Copy(src, dst, send_sem, recv_sem, device)

    def send_weights(e, i):
        if once("w", e):
            for copy in w_in[e]:
                copy.wait()
        for d in range(2):
            half = i if d == 0 else 1 - i
            rows = pl.ds(half * HALF, HALF)
            send(
                ("w", e, d, half), wbuf.at[0, e, rows, :], wbuf.at[2 - d, e, rows, :],
                w_s.at[e, d, half], w_r.at[e, d, half], at_y(1 if d == 0 else 3),
            )

    def pass_weights(e, d):
        copies["w", e, d, d].wait()
        rows = pl.ds(d * HALF, HALF)
        send(
            ("f", e, d), wbuf.at[2 - d, e, rows, :], wbuf.at[3, e, rows, :],
            wf_s.at[e, d], wf_r.at[e, d], at_y(1 if d == 0 else 3),
        )

    def weights_done(e, piece):
        if piece == 1:
            for d in range(2):
                for half in range(2):
                    copies["w", e, d, half].wait()
        elif piece == 2:
            for d in range(2):
                copies["f", e, d].wait()

    count = tok_ref.shape[0]
    start = pl.multiple_of(z * count, LANES)
    rank = []

    def find_ranks():
        above = lax.broadcasted_iota(jnp.int32, (count, count), 0)
        right = lax.broadcasted_iota(jnp.int32, (count, count), 1)
        before = (above < right).astype(jnp.float32).astype(jnp.bfloat16)
        token = lax.broadcasted_iota(jnp.int32, (1, ids_ref.shape[1]), 1)
        for e in range(EXPERTS):
            named = (ids_ref[0:1, :] == e) | (ids_ref[1:2, :] == e)
            ahead = jnp.sum((named & (token < start)).astype(jnp.float32), axis=1, keepdims=True)
            lanes = pl.ds(start, count)
            own = (ids_ref[0:1, lanes] == e) | (ids_ref[1:2, lanes] == e)
            ones = jnp.broadcast_to(own.astype(jnp.float32), (16, count)).astype(jnp.bfloat16)
            within = jnp.dot(ones, before, preferred_element_type=jnp.float32)[0:1]
            rank.append(jnp.where(own, (within + ahead).astype(jnp.int32), -1))

    def slot_start(c, r):
        to_hi = xh if CHUNKS[c][1] else 1 - xh
        to_core = core if r else 1 - core
        return (col * 4 + to_hi * 2 + to_core) * BLOCK

    def place_rows(c):
        if once("tok"):
            tok_in.wait()
        index = lax.broadcasted_iota(jnp.int32, (BLOCK, count), 0)
        slot = jnp.concatenate([index + slot_start(c, 0), index + slot_start(c, 1)], axis=0)
        pick = (slot == rank[CHUNKS[c][0]]).astype(jnp.float32).astype(jnp.bfloat16)
        for f in range(2):
            placed[c, :, f * HALF : (f + 1) * HALF] = jnp.dot(
                pick, tok_ref[:, f * HALF : (f + 1) * HALF], preferred_element_type=jnp.float32
            ).astype(jnp.bfloat16)

    def owner_lanes(k):
        return pl.ds(pl.multiple_of((k % 4) * QUARTER, LANES), QUARTER)

    def owner_rows(c, k):
        return placed.at[c, pl.ds(pl.multiple_of((k // 4) * BLOCK, 16), BLOCK), owner_lanes(k)]

    def reduce_send(c, d, s, src, hops):
        send(
            ("r", c, d, s), src, sums.at[c, d, s - 1],
            rs_s.at[c, d, s - 1], rs_r.at[c, d, s - 1], at_row((1 - 2 * d) * hops),
        )

    def reduce_step(c, d, s):
        sign, steps = 1 - 2 * d, ring_steps(c % 2)[d]
        if once("p", c):
            place_rows(c)

        def rows_for(distance):
            return owner_rows(c, lax.rem(z + sign * distance + ROWS, ROWS))

        if c not in TREES:
            src = rows_for(steps - s + 1)
            if s > 1:
                copies["r", c, d, s - 1].wait()
                sums[c, d, s - 2] = sums[c, d, s - 2] + src[...]
                src = sums.at[c, d, s - 2]
            reduce_send(c, d, s, src, 1)
        elif s == 1:
            reduce_send(c, d, 1, rows_for(3), 1)
            if steps == 4:
                reduce_send(c, d, 2, rows_for(4), 2)
            reduce_send(c, d, 4, rows_for(1), 1)
        else:
            copies["r", c, d, 1].wait()
            total = sums[c, d, 0] + rows_for(2)[...]
            if steps == 4:
                copies["r", c, d, 2].wait()
                total = total + sums[c, d, 1]
            sums[c, d, 0] = total
            reduce_send(c, d, 3, sums.at[c, d, 0], 2)

    def slot_rows(c, k, side):
        first = pl.multiple_of((k // 4) * (2 * BLOCK) + side * BLOCK, 16)
        return slots.at[c, pl.ds(first, BLOCK), owner_lanes(k)]

    def both_sides(c, k):
        first = pl.multiple_of((k // 4) * (2 * BLOCK), 16)
        return slots.at[c, pl.ds(first, 2 * BLOCK), owner_lanes(k)]

    def to_pair(c, i, k):
        rows = slot_rows(c, k, xl)
        send(("x", c, i), rows, rows, x_s.at[c, i], x_r.at[c, i], pair)

    def finish_reduce(c):
        total = owner_rows(c, z)[...]
        for d in range(2):
            for s in (3, 4) if c in TREES else (ring_steps(c % 2)[d],):
                copies["r", c, d, s].wait()
                total = total + sums[c, d, s - 1]
        mine = slot_rows(c, z, xl)
        mine[...] = total
        if c in SIDEWAYS:
            for d in range(2):
                gather_send(c, d, 1)
        to_pair(c, 0, z)

    def gather_block(c, d, distance):
        return lax.rem(z - (1 - 2 * d) * distance + ROWS, ROWS)

    def gather_copy(c, d, s, distance, hops):
        k = gather_block(c, d, distance)
        rows = slot_rows(c, k, xl) if c in SIDEWAYS else both_sides(c, k)
        send(
            ("a", c, d, s), rows, rows, ag_s.at[c, d, s - 1], ag_r.at[c, d, s - 1],
            at_row((1 - 2 * d) * hops),
        )

    def gather_send(c, d, s):
        steps = ring_steps(1 - c % 2)[d]
        if c not in SPREADS:
            if s <= steps:
                gather_copy(c, d, s, s - 1, 1)
        elif s == 1:
            gather_copy(c, d, 1, 0, 1)
            gather_copy(c, d, 2, 0, 2)
        elif s == 3:
            gather_copy(c, d, 3, 2, 1)
            if steps == 4:
                gather_copy(c, d, 4, 2, 2)

    def gather_step(c, d, s):
        if s == 1:
            copies["x", c, 0].wait()
        else:
            copies["a", c, d, s - 1].wait()
        gather_send(c, d, s)
        if c in SIDEWAYS:
            to_pair(c, 1 + d * ring_steps(1 - c % 2)[0] + s - 2, gather_block(c, d, s - 1))

    def slots_done(c, own_only=False):
        for d in range(2):
            for s in range(ring_steps(1 - c % 2)[d]):
                copies["a", c, d, s + 1].wait()
        if not own_only:
            for i in range(8 if c in SIDEWAYS else 1):
                copies["x", c, i].wait()

    def project_side(c, piece, s):
        e = CHUNKS[c][0]
        first, number = PIECES[piece]
        side = xl if s == 0 else 1 - xl
        slots_done(c, s == 0)
        weights_done(e, piece)
        low = pl.multiple_of(side * BLOCK, 16)
        rows = jnp.concatenate(
            [slots[c, pl.ds(low, BLOCK), :], slots[c, pl.ds(low + 2 * BLOCK, BLOCK), :]], axis=0
        )
        for b in range(first, first + number):
            total = jnp.dot(rows, wbuf[b, e], preferred_element_type=jnp.float32)
            for r in range(2):
                part[c, r, b, side] = total[r * BLOCK : (r + 1) * BLOCK]
        span = pl.ds(first, number)
        send(
            ("c", c, piece, s), part.at[c, 0, span, side], from_core.at[c, span, side],
            c_s.at[c, piece, s], c_r.at[c, piece, s], other_core,
        )

    def to_hi_side(c, piece, s):
        e = CHUNKS[c][0]
        first, number = PIECES[piece]
        side = xl if s == 0 else 1 - xl
        copies["c", c, piece, s].wait()
        for b in range(first, first + number):
            part[c, 1, b, side] = part[c, 1, b, side] + from_core[c, b, side]
        span = pl.ds(first, number)
        send(
            ("h", e, piece, s), part.at[c, 1, span, side], from_hi.at[e, span, side],
            h_s.at[e, piece, s], h_r.at[e, piece, s], other_hi,
        )

    def project(c, piece, *rows):
        e = CHUNKS[c][0]
        first, number = PIECES[piece]
        slots_done(c)
        weights_done(e, piece)
        top, span = rows[0] * 2 * BLOCK, len(rows) * 2 * BLOCK
        for b in range(first, first + number):
            total = jnp.dot(
                slots[c, top : top + span, :], wbuf[b, e], preferred_element_type=jnp.float32
            )
            for i, row in enumerate(rows):
                for side in range(2):
                    at = (i * 2 + side) * BLOCK
                    part[c, row, b, side] = total[at : at + BLOCK]
        if 0 in rows:
            span = pl.ds(first, number)
            send(
                ("c", c, piece, 0), part.at[c, 0, span], from_core.at[c, span],
                c_s.at[c, piece, 0], c_r.at[c, piece, 0], other_core,
            )

    def to_hi(c, piece):
        e = CHUNKS[c][0]
        first, number = PIECES[piece]
        copies["c", c, piece, 0].wait()

        for b in range(first, first + number):
            for side in range(2):
                part[c, 1, b, side] = part[c, 1, b, side] + from_core[c, b, side]

        span = pl.ds(first, number)
        send(
            ("h", e, piece, 0), part.at[c, 1, span], from_hi.at[e, span],
            h_s.at[e, piece, 0], h_r.at[e, piece, 0], other_hi,
        )

    def hidden(e, side, b):
        c = CHUNKS.index((e, 1))
        total = part[c, 1, b, side] + from_core[c, b, side] + from_hi[e, b, side]
        gate, up = total[:, :LANES], total[:, LANES:]
        return (gate / (1.0 + jnp.exp(-gate)) * up).astype(jnp.bfloat16)

    def positions(piece):
        first, number = PIECES[piece]
        return range(first, first + number), pl.ds(first * LANES, number * LANES)

    def finish_out(e, piece):
        for s in range(2 if CHUNKS.index((e, 0)) in SIDEWAYS else 1):
            copies["h", e, piece, s].wait()
        copies["c", CHUNKS.index((e, 1)), piece, 0].wait()
        blocks, lanes = positions(piece)
        for b in blocks:
            sent[e, :, b * LANES : (b + 1) * LANES] = hidden(e, 1 - xl, b)
        send(
            ("o", e, piece), sent.at[e, :, lanes], back.at[e, :, lanes],
            o_s.at[e, piece], o_r.at[e, piece], pair,
        )

    def finish_own(e, piece):
        for b in positions(piece)[0]:
            out_ref[e, :, out_lanes(xl, b)] = hidden(e, xl, b)

    def out_lanes(side, b):
        return pl.ds(pl.multiple_of((side * 4 + lax.rem(y + Y_STEP[b], 4)) * LANES, LANES), LANES)

    def take_back(e, piece):
        copies["o", e, piece].wait()
        for b in positions(piece)[0]:
            out_ref[e, :, out_lanes(1 - xl, b)] = back[e, :, b * LANES : (b + 1) * LANES]

    find_ranks()
    for c in range(2):
        once("p", c)
        place_rows(c)
    pl.semaphore_wait(barrier, len(partners))
    acts = {
        "w": send_weights, "f": pass_weights, "r": reduce_step, "t": finish_reduce, "a": gather_step,
        "p": project, "h": to_hi, "q": project_side, "k": to_hi_side, "o": finish_out, "m": finish_own, "b": take_back,
    }
    for step in PLAN:
        acts[step[0]](*map(int, step[1:]))
    for copy in copies.values():
        copy.copy.wait_send()


def shards(tokens, expert_ids, w_gate, w_up):
    bf16, f32 = jnp.bfloat16, jnp.float32
    vmem, dma = pltpu.VMEM, pltpu.SemaphoreType.DMA
    chunks = len(CHUNKS)
    return pl.pallas_call(
        kernel,
        name="experts",
        out_shape=jax.ShapeDtypeStruct((EXPERTS, BLOCK, 1024), bf16),
        in_specs=[pl.BlockSpec(memory_space=pltpu.VMEM)] + [pl.BlockSpec(memory_space=pl.ANY)] * 3,
        out_specs=pl.BlockSpec(memory_space=pltpu.VMEM),
        scratch_shapes=[
            vmem(tokens.shape, bf16),
            vmem((4, EXPERTS, DEPTH, 2 * LANES), bf16),
            vmem((chunks, 2 * BLOCK, DEPTH), bf16),
            vmem((chunks, 2, 4, BLOCK, QUARTER), bf16),
            vmem((chunks, 4 * BLOCK, DEPTH), bf16),
            vmem((chunks, 2, 4, 2, BLOCK, 2 * LANES), f32),
            vmem((chunks, 4, 2, BLOCK, 2 * LANES), f32),
            vmem((EXPERTS, 4, 2, BLOCK, 2 * LANES), f32),
            vmem((EXPERTS, BLOCK, 4 * LANES), bf16),
            vmem((EXPERTS, BLOCK, 4 * LANES), bf16),
            dma((5,)),
            dma((EXPERTS, 2, 2)), dma((EXPERTS, 2, 2)),
            dma((EXPERTS, 2)), dma((EXPERTS, 2)),
            dma((chunks, 2, 4)), dma((chunks, 2, 4)),
            dma((chunks, 8)), dma((chunks, 8)),
            dma((chunks, 2, 4)), dma((chunks, 2, 4)),
            dma((chunks, 3, 2)), dma((chunks, 3, 2)),
            dma((EXPERTS, 3, 2)), dma((EXPERTS, 3, 2)),
            dma((EXPERTS, 3)), dma((EXPERTS, 3)),
        ],
        compiler_params=pltpu.CompilerParams(
            collective_id=0, has_side_effects=True, vmem_limit_bytes=55920000
        ),
    )(expert_ids.T, tokens, w_gate, w_up)


def solution(mesh):
    in_specs = (
        P("row", "layer"),
        P(),
        P(None, "layer", ("row", "col")),
        P(None, "layer", ("row", "col")),
    )
    out_specs = P(None, ("col", "layer"), "row")
    return jax.shard_map(shards, mesh=mesh, in_specs=in_specs, out_specs=out_specs, check_vma=False)
```
